512 devices in a mesh: dp: 64 (over x, z_lo, core), mp: 8 (over z_hi, y).
Axes of the slice: x: 4, y: 4, z: 16 (z_hi: 2, z_lo: 8; z = z_hi * 8 + z_lo), core: 2. Of those that a mesh axis runs over, the one named last changes fastest.
Arguments:
- tokens: bfloat16 [768, 4608], P('dp', 'mp'), may hold values from -6 to 6
- frozen_weight: bfloat16 [2, 4608, 36864], P(None, 'mp', 'dp'), may hold values from -36 to 36
- adapter_down: bfloat16 [2, 16, 4608], P(None, None, 'mp'), may hold values from -1.5 to 1.5
- adapter_up: bfloat16 [2, 16, 36864], P(None, None, 'dp'), may hold values from -3 to 3
- magnitude: float32 [2, 36864], P(None, 'dp'), may hold values from 0.5 to 2
- hidden_gradient: bfloat16 [768, 36864], P('mp', 'dp'), may hold values from -0.59765625 to 0.59765625
Outputs:
- hidden: bfloat16 [768, 36864], P('mp', 'dp')
- token_gradient: float32 [768, 4608], P('dp', 'mp')
- adapter_down_gradient: float32 [2, 16, 4608], P(None, None, 'mp')
- adapter_up_gradient: float32 [2, 16, 36864], P(None, None, 'dp')
- magnitude_gradient: float32 [2, 36864], P(None, 'dp')
The draws below stay inside these ranges and needn't reach their ends.
All inputs are finite; a program needn't handle non-finite values.
Results may differ from the reference program's by a relative error of at most 0.023.
Values may be sent and summed in bfloat16 or wider, within the bound.
A program may use at most 64 MiB of HBM per device.

```python
import math
import jax
import jax.numpy as jnp
from jax import lax

MODEL_WIDTH = 4608
HIDDEN_UNITS = 36864
ADAPTER_RANK = 16
TOKENS = 768
N_DP = 64
N_MP = 8


def draw_frozen_weight(key, part):
    row_key = jax.random.fold_in(key, 11)
    col_key = jax.random.fold_in(key, 12)
    entry_key = jax.random.fold_in(key, 13)
    positions = jnp.arange(MODEL_WIDTH, dtype=jnp.float32) / (MODEL_WIDTH - 1)
    row_ramp = jnp.sqrt(1.0 + 2.0 * positions).reshape(1, MODEL_WIDTH, 1)
    row_scale = row_ramp * jnp.exp(jax.random.uniform(row_key, (2, MODEL_WIDTH, 1), jnp.float32, 0.0, 1.7917595))
    col_scale = jnp.exp(jax.random.uniform(col_key, (2, 1, HIDDEN_UNITS), jnp.float32, -1.2039728, 1.0986123))
    entries = jnp.clip(jax.random.normal(entry_key, (2, MODEL_WIDTH, HIDDEN_UNITS), jnp.float32), -5.0, 5.0)
    return (entries * row_scale * col_scale / 4.4).astype(jnp.bfloat16)


def steps_of(key, dims, pieces, smallest, high):
    def one(dim, shards_of):
        draws = jax.random.uniform(jax.random.fold_in(jax.random.fold_in(key, 6), dim), (shards_of,), jnp.float32, smallest / len(pieces), high / len(pieces))
        return jnp.repeat(jnp.exp(draws), dims[dim] // shards_of).reshape((-1,) + (1,) * (len(dims) - dim - 1))

    gain = one(*pieces[0])
    for cut in pieces[1:]:
        gain = gain * one(*cut)
    return gain


def scatter_about(rng, shape, deviation, bound, cuts=(), kind=jnp.bfloat16):
    level = steps_of(rng, shape, cuts, -0.22, 0.18) if cuts else 1.0
    drawn = jax.random.normal(rng, shape, jnp.float32) * deviation * level
    return jnp.minimum(jnp.maximum(drawn, -bound), bound).astype(kind)


def setup_inputs(seed: int = 0) -> dict:
    key_of = jax.random.split(jax.random.key(seed), 7)
    tokens = scatter_about(key_of[0], (TOKENS, MODEL_WIDTH), 1.0, 6.0, ((0, 64), (1, 8)))
    frozen_weight = draw_frozen_weight(jax.random.fold_in(key_of[6], 71), 0)
    adapter_down = scatter_about(key_of[2], (2, ADAPTER_RANK, MODEL_WIDTH), ADAPTER_RANK ** -0.5, 1.5, ((2, 8),))
    adapter_up = scatter_about(key_of[3], (2, ADAPTER_RANK, HIDDEN_UNITS), 0.5, 3.0, ((2, 64),))
    magnitude = jnp.clip(jnp.exp(math.log(2.0) - 1.3862944 * jax.random.uniform(key_of[4], (2, HIDDEN_UNITS), jnp.float32) ** steps_of(key_of[4], (2, HIDDEN_UNITS), ((1, 64),), -0.2, 0.2)), 0.5, 2.0)
    hidden_gradient = scatter_about(key_of[5], (TOKENS, HIDDEN_UNITS), 0.1, 0.59765625, ((0, 8), (1, 64)))
    return {"tokens": tokens, "frozen_weight": frozen_weight, "adapter_down": adapter_down, "adapter_up": adapter_up, "magnitude": magnitude, "hidden_gradient": hidden_gradient}


LOWRANK_SCALE = 2.0
EPSILON = 1e-06
MATMUL_ACCURACY = lax.Precision.HIGHEST

def gelu_pair(source):
    cubic_term = source + 0.044715 * source * source * source
    tangent = jnp.tanh(0.7978845608028654 * cubic_term)
    result = 0.5 * source * (1.0 + tangent)
    derivative = 0.5 * (1.0 + tangent) + 0.5 * source * (1.0 - tangent * tangent) * 0.7978845608028654 * (1.0 + 0.134145 * source * source)
    return (result, derivative)

def group_product(tokens, weights):
    group_depth = MODEL_WIDTH // N_MP
    col_count = weights.shape[2]

    def add_group(running, group_index):
        offset = group_index * group_depth
        token_cols = lax.dynamic_slice_in_dim(tokens, offset, group_depth, 1).astype(jnp.float32)
        weight_rows = lax.dynamic_slice_in_dim(weights, offset, group_depth, 1).astype(jnp.float32)
        partial_sum = jnp.einsum('td,kdf->ktf', token_cols, weight_rows, precision=MATMUL_ACCURACY)
        rounded = lax.optimization_barrier(partial_sum.astype(jnp.bfloat16))
        return (running + rounded.astype(jnp.float32), None)
    initial = jnp.zeros((2, TOKENS, col_count), jnp.float32)
    return lax.scan(add_group, initial, jnp.arange(N_MP, dtype=jnp.int32))[0]

def combined_block(frozen_block, adapter_down, adapter_up_block):
    lowrank_delta = jnp.einsum('ipq,iph->iqh', adapter_down.astype(jnp.float32), adapter_up_block.astype(jnp.float32), precision=MATMUL_ACCURACY)
    return frozen_block.astype(jnp.float32) + LOWRANK_SCALE * lowrank_delta

def reference(tokens, frozen_weight, adapter_down, adapter_up, magnitude, hidden_gradient):
    column_blocks = N_DP
    block_columns = HIDDEN_UNITS // column_blocks
    weight_blocks = jnp.moveaxis(frozen_weight.reshape(2, MODEL_WIDTH, column_blocks, block_columns), 2, 0)
    adapter_up_blocks = jnp.moveaxis(adapter_up.reshape(2, ADAPTER_RANK, column_blocks, block_columns), 2, 0)
    down_broad = adapter_down.astype(jnp.float32)

    def norm_pass(block_pieces):
        combined_weight = combined_block(block_pieces[0], adapter_down, block_pieces[1])
        squares = lax.optimization_barrier(jnp.sum(combined_weight * combined_weight, axis=1))
        cross_part = jnp.einsum('krd,kdf->krf', down_broad, combined_weight, precision=MATMUL_ACCURACY)
        return (squares, cross_part)
    squares, cross_parts = lax.map(norm_pass, (weight_blocks, adapter_up_blocks))
    square_sum = jnp.moveaxis(squares, 0, 1).reshape(2, HIDDEN_UNITS)
    mixed_sum = jnp.moveaxis(cross_parts, 0, 2).reshape(2, ADAPTER_RANK, HIDDEN_UNITS)
    col_norm = jnp.sqrt(square_sum + EPSILON)
    col_ratio = magnitude / col_norm
    token_lowrank = group_product(tokens, jnp.swapaxes(adapter_down, 1, 2)).astype(jnp.bfloat16)
    frozen_matrix = group_product(tokens, frozen_weight)
    unscaled_output = frozen_matrix + LOWRANK_SCALE * jnp.einsum('hls,hse->hle', token_lowrank.astype(jnp.float32), adapter_up.astype(jnp.float32), precision=MATMUL_ACCURACY)
    gate_proj = unscaled_output[0] * col_ratio[0]
    up_proj = unscaled_output[1] * col_ratio[1]
    activated, derivative = gelu_pair(gate_proj)
    hidden = (activated * up_proj).astype(jnp.bfloat16)
    cotangent = hidden_gradient.astype(jnp.float32)
    grad_out = jnp.stack([cotangent * up_proj * derivative, cotangent * activated])
    moment = lax.optimization_barrier(jnp.sum(grad_out * unscaled_output, axis=1))
    magnitude_gradient = moment / col_norm
    frozen_term = -magnitude * moment / (col_norm * col_norm * col_norm)
    prescale_gradient = (grad_out * col_ratio[:, None, :]).astype(jnp.bfloat16)
    lowrank_gradient = jnp.stack([jnp.dot(prescale_gradient[pair_member], adapter_up[pair_member].T, preferred_element_type=jnp.float32) for pair_member in range(2)]).astype(jnp.bfloat16)
    adapter_up_gradient = LOWRANK_SCALE * (jnp.einsum('hmu,hmq->huq', token_lowrank.astype(jnp.float32), prescale_gradient.astype(jnp.float32), precision=MATMUL_ACCURACY) + mixed_sum * frozen_term[:, None, :])
    weighted_adapter_up = adapter_up.astype(jnp.float32) * frozen_term[:, None, :]
    weighted_blocks = jnp.moveaxis(weighted_adapter_up.reshape(2, ADAPTER_RANK, column_blocks, block_columns), 2, 0)

    def spread_pass(running, block_pieces):
        combined_weight = combined_block(block_pieces[0], adapter_down, block_pieces[1])
        return (running + jnp.einsum('krf,kdf->krd', block_pieces[2], combined_weight, precision=MATMUL_ACCURACY), None)
    broadcast_value = lax.scan(spread_pass, jnp.zeros((2, ADAPTER_RANK, MODEL_WIDTH), jnp.float32), (weight_blocks, adapter_up_blocks, weighted_blocks))[0]
    adapter_down_gradient = LOWRANK_SCALE * (jnp.einsum('ijp,jv->ipv', lowrank_gradient.astype(jnp.float32), tokens.astype(jnp.float32), precision=MATMUL_ACCURACY) + broadcast_value)
    token_gradient = jnp.zeros((TOKENS, MODEL_WIDTH), jnp.float32)
    for pair_member in range(2):
        token_gradient = token_gradient + jnp.dot(prescale_gradient[pair_member], frozen_weight[pair_member].T, preferred_element_type=jnp.float32) + LOWRANK_SCALE * jnp.dot(lowrank_gradient[pair_member], adapter_down[pair_member], preferred_element_type=jnp.float32)
    return (hidden, token_gradient, adapter_down_gradient, adapter_up_gradient, magnitude_gradient)
```

```python
import functools

import jax
import jax.numpy as jnp
from jax import lax
from jax.experimental import pallas as pl
from jax.experimental.pallas import tpu as pltpu
from jax.sharding import PartitionSpec as P

SCALE = 2.0
EPSILON = 1e-06
MESH = pl.DeviceIdType.MESH
F32 = jnp.float32
BF16 = jnp.bfloat16
NT = (((1,), (1,)), ((), ()))
TN = (((0,), (0,)), ((), ()))
NN = (((1,), (0,)), ((), ()))

NX, NY, NZ, NH, NC = 4, 4, 8, 2, 2
ROWS = 96
MINI = 12
WIDE = 576
RANK = 16
STEP = 32
PARTS = ROWS // STEP
CHUNKS = PARTS * NH
BLOCK = NY * STEP


def dot(a, b, dims=NN):
    return lax.dot_general(a, b, dims, preferred_element_type=F32)


def wide_dot(a, b, dims=NN):
    total = None
    for _ in range(3):
        term = a.astype(BF16)
        a = a - term.astype(F32)
        value = dot(term, b, dims)
        total = value if total is None else total + value
    return total


def gelu_pair(source):
    square = source * source
    tangent = jnp.tanh(0.7978845608028654 * (source + 0.044715 * source * square))
    half = 0.5 * (1.0 + tangent)
    slope = half + 0.5 * source * (1.0 - tangent * tangent) * 0.7978845608028654 * (
        1.0 + 0.134145 * square
    )
    return source * half, slope


def kernel(
    tok, w, down, up, mag, cot,
    hid, tg, dg, ug, mg,
    zin, zflat, xb, sq, low_t, up_wide, part, ypart, zpart_out, zpart_in, cots, grad,
    mom, mom_all, acc_d, acc_u, cross, tb, tpair, tsum, tx, tflat, zout, zback,
    d_pair_out, d_pair_in, d_x, d_z, d_last, u_y, u_z,
    zs, zr, xs, xr, cs, cr, qs, qr, ts, tr, ps, pr, ss, sr, gs, gr, ms, mr,
    fs, fr, fxs, fxr, bs, br, ds1, dr1, ds2, dr2, ds3, dr3, ds4, dr4, us1, ur1, us2, ur2,
):
    dp = lax.axis_index("dp")
    mp = lax.axis_index("mp")
    c = lax.rem(dp, NC)
    zl = lax.rem(dp // NC, NZ)
    x = dp // (NC * NZ)
    y = lax.rem(mp, NY)
    zh = mp // NY
    half = zl // 4
    slot = lax.rem(zl, 4) * 2 + c
    mine = half == c

    def at(x=x, zl=zl, c=c, zh=zh, y=y):
        return ((x * NZ + zl) * NC + c, zh * NY + y)

    def send(src, dst, s, r, device):
        return pltpu.make_async_remote_copy(
            src_ref=src, dst_ref=dst, send_sem=s, recv_sem=r,
            device_id=device, device_id_type=MESH,
        )

    partner = at(c=1 - c)
    across = at(zh=1 - zh)
    xnext = [lax.rem(x + d, NX) for d in range(1, NX)]
    ynext = [lax.rem(y + d, NY) for d in range(1, NY)]
    xdev = [at(x=v) for v in xnext]
    ydev = [at(y=v) for v in ynext]

    barrier = pltpu.get_barrier_semaphore()
    greeted = 0
    for k in range(1, NZ):
        for other in (c, 1 - c):
            pl.semaphore_signal(
                barrier, 1, device_id=at(zl=lax.rem(zl + k, NZ), c=other), device_id_type=MESH
            )
            greeted += 1
    for device in [partner, across] + xdev + ydev + [at(zh=1 - zh, y=v) for v in ynext]:
        pl.semaphore_signal(barrier, 1, device_id=device, device_id_type=MESH)
        greeted += 1

    for k in range(2):
        merged = w[k].astype(F32) + SCALE * dot(down[k], up[k], TN)
        sq[mp, pl.ds(k, 1), :] = jnp.sum(merged * merged, axis=0, keepdims=True)

    pl.semaphore_wait(barrier, greeted)

    zcopies = []
    for t in range(NZ):
        zcopies.append(send(tok, zin.at[slot], zs.at[t], zr.at[slot], at(zl=t, c=half)))

        @pl.when(jnp.logical_not(jnp.logical_and(mine, zl == t)))
        def _():
            zcopies[t].start()

    @pl.when(mine)
    def _():
        zin[slot] = tok[...]

    qcopies = []
    for i, device in enumerate(ydev + [across] + [at(zh=1 - zh, y=v) for v in ynext]):
        qcopies.append(send(sq.at[mp], sq.at[mp], qs.at[i], qr.at[mp], device))
        qcopies[-1].start()

    cots[zh] = cot[...]
    for k in range(2):
        up_wide[k] = jnp.zeros((2 * RANK, WIDE), BF16)
        up_wide[k, RANK * k : RANK * (k + 1), :] = (SCALE * up[k].astype(F32)).astype(BF16)
        gram = dot(down[k], down[k], NT)
        cross[k] = dot(down[k], w[k]) + SCALE * wide_dot(gram, up[k])
    mom[...] = jnp.zeros_like(mom)
    acc_d[...] = jnp.zeros_like(acc_d)
    acc_u[...] = jnp.zeros_like(acc_u)
    down_both = down[...].reshape(2 * RANK, WIDE)

    for s in range(8):

        @pl.when(jnp.logical_not(jnp.logical_and(mine, slot == s)))
        def _():
            send(tok, zin.at[s], zs.at[0], zr.at[s], partner).wait_recv()

        zflat[MINI * s : MINI * (s + 1), :] = zin[s].astype(F32)
    own = x * 2 + c
    xb[own] = zflat[...].astype(BF16)

    xcopies = []
    for d in range(3):
        xcopies.append(send(xb.at[own], xb.at[own], xs.at[d], xr.at[x], xdev[d]))
        xcopies[-1].start()
    ccopies = [send(xb.at[own], xb.at[own], cs.at[x], cr.at[x], partner)]
    ccopies[-1].start()
    tcopy = send(cot, cots.at[zh], ts, tr, across)
    tcopy.start()
    for v in [lax.rem(x + 3, NX), xnext[0], xnext[1]]:
        block = xb.at[v * 2 + c]
        send(block, block, xs.at[0], xr.at[v], partner).wait_recv()
        ccopies.append(send(block, block, cs.at[v], cr.at[v], partner))
        ccopies[-1].start()
    for v in range(NX):
        block = xb.at[v * 2 + 1 - c]
        send(block, block, cs.at[0], cr.at[v], partner).wait_recv()

    def place(q):
        return q // NH, lax.rem(q, NH) if not isinstance(q, int) else q % NH

    def rows_of(q):
        r, h = place(q)
        return xb[NY * h : NY * (h + 1), STEP * r : STEP * (r + 1), :].reshape(BLOCK, WIDE)

    pcopies = []

    def products(q):
        lhs = rows_of(q)
        low = dot(lhs, down_both, NT).astype(BF16)
        low_t[q] = dot(down_both, lhs, NT).astype(BF16)
        for k in range(2):
            value = dot(lhs, w[k]) + dot(low, up_wide[k])
            part[q, :, k] = value.astype(BF16).reshape(NY, STEP, WIDE)
        for d in range(3):
            pcopies.append(
                send(part.at[q, ynext[d]], ypart.at[q, d], ps.at[q, d], pr.at[q, d], ydev[d])
            )
            pcopies[-1].start()

    scopies = []

    def over_y(q):
        total = part[q, y].astype(F32)
        for d in range(3):
            send(part.at[q, y], ypart.at[q, d], ps.at[q, d], pr.at[q, d], partner).wait_recv()
            total = total + ypart[q, d].astype(F32)
        zpart_out[q] = total.astype(BF16)
        scopies.append(send(zpart_out.at[q], zpart_in.at[q], ss.at[q], sr.at[q], across))
        scopies[-1].start()

    products(0)
    products(1)
    for q in range(CHUNKS):
        over_y(q)
        if q + 2 < CHUNKS:
            products(q + 2)

    for device in range(NH * NY):

        @pl.when(device != mp)
        def _():
            send(sq.at[device], sq.at[device], qs.at[0], qr.at[device], partner).wait_recv()

    norm_square = sq[0]
    for device in range(1, NH * NY):
        norm_square = norm_square + sq[device]
    norm = jnp.sqrt(norm_square + EPSILON)
    ratio = mag[...] / norm
    tcopy.wait_recv()

    gcopies = []

    def activate(q):
        r, h = place(q)
        rows = slice(STEP * r, STEP * (r + 1))
        send(zpart_out.at[q], zpart_in.at[q], ss.at[q], sr.at[q], partner).wait_recv()
        pre = [zpart_out[q, k].astype(F32) + zpart_in[q, k].astype(F32) for k in range(2)]
        gate = pre[0] * ratio[0:1]
        lift = pre[1] * ratio[1:2]
        active, slope = gelu_pair(gate)

        @pl.when(zh == h)
        def _():
            hid[rows, :] = (active * lift).astype(BF16)

        g = cots[h, rows, :].astype(F32)
        outs = [g * lift * slope, g * active]
        for k in range(2):
            mom[k : k + 1, :] += jnp.sum(outs[k] * pre[k], axis=0, keepdims=True)
            grad[q, y, k] = (outs[k] * ratio[k : k + 1]).astype(BF16)
        for d in range(3):
            gcopies.append(
                send(grad.at[q, y], grad.at[q, y], gs.at[q, d], gr.at[q, y], ydev[d])
            )
            gcopies[-1].start()

    fcopies = []

    def backward(q):
        for d in range(3):
            block = grad.at[q, ynext[d]]
            send(block, block, gs.at[q, d], gr.at[q, ynext[d]], partner).wait_recv()
        lhs = rows_of(q)
        total = None
        for k in range(2):
            g = grad[q, :, k].reshape(BLOCK, WIDE)
            low = dot(g, up[k], NT).astype(BF16)
            low_rows = dot(up[k], g, NT).astype(BF16)
            value = dot(g, w[k], NT) + SCALE * dot(low, down[k])
            total = value if total is None else total + value
            acc_d[k] += dot(low_rows, lhs)
            acc_u[k] += dot(low_t[q, RANK * k : RANK * (k + 1), :], g)
        tb[q] = total.astype(BF16).reshape(2, 2, STEP, WIDE)
        for j in range(2):
            fcopies.append(
                send(tb.at[q, j, 1 - c], tpair.at[q, j], fs.at[q, j], fr.at[q, j], partner)
            )
            fcopies[-1].start()

    fxcopies = []

    def over_cores(q):
        r, h = place(q)
        for j in range(2):
            send(tb.at[q, j, c], tpair.at[q, j], fs.at[q, j], fr.at[q, j], partner).wait_recv()
            tsum[q, j] = (tb[q, j, c].astype(F32) + tpair[q, j].astype(F32)).astype(BF16)
            target = NH * h + j
            copy = send(
                tsum.at[q, j], tx.at[r, x], fxs.at[q, j], fxr.at[r, x], at(x=target)
            )
            fxcopies.append((target, copy))

            @pl.when(x != target)
            def _():
                copy.start()

    for q in range(CHUNKS):
        activate(q)
        if q == CHUNKS - 1:
            mom_all[y] = mom[...]
            mcopies = []
            for d in range(3):
                mcopies.append(send(mom_all.at[y], mom_all.at[y], ms.at[d], mr.at[y], ydev[d]))
                mcopies[-1].start()
        if q:
            over_cores(q - 1)
        backward(q)

    for v in ynext:
        send(mom_all.at[v], mom_all.at[v], ms.at[0], mr.at[v], partner).wait_recv()
    moment = mom_all[0]
    for v in range(1, NY):
        moment = moment + mom_all[v]
    mg[...] = moment / norm
    term = -mag[...] * moment / (norm * norm * norm)
    for k in range(2):
        u_y[y, RANK * k : RANK * (k + 1), :] = (
            SCALE * (acc_u[k] + cross[k] * term[k : k + 1])
        ).astype(BF16)
    u1 = []
    for d in range(3):
        u1.append(send(u_y.at[y], u_y.at[y], us1.at[d], ur1.at[y], ydev[d]))
        u1[-1].start()
    for k in range(2):
        weighted = up[k].astype(F32) * term[k : k + 1]
        spread = wide_dot(weighted, w[k], NT)
        spread = spread + SCALE * wide_dot(wide_dot(weighted, up[k], NT), down[k])
        acc_d[k] = SCALE * (acc_d[k] + spread)
    d_pair_out[...] = acc_d[1 - c].astype(BF16)
    d1 = send(d_pair_out, d_pair_in, ds1, dr1, partner)
    d1.start()
    over_cores(CHUNKS - 1)

    d1.wait_recv()
    d_x[x] = (acc_d[c] + d_pair_in[...].astype(F32)).astype(BF16)
    d2 = []
    for d in range(3):
        d2.append(send(d_x.at[x], d_x.at[x], ds2.at[d], dr2.at[x], xdev[d]))
        d2[-1].start()

    for v in ynext:
        send(u_y.at[v], u_y.at[v], us1.at[0], ur1.at[v], partner).wait_recv()
    total_u = u_y[0].astype(F32)
    for v in range(1, NY):
        total_u = total_u + u_y[v].astype(F32)
    u_z[zh] = total_u.astype(BF16)
    u2 = send(u_z.at[zh], u_z.at[zh], us2, ur2.at[zh], across)
    u2.start()

    for r in range(PARTS):
        total = tsum[NH * r + x // 2, lax.rem(x, 2)].astype(F32)
        for v in xnext:
            send(tx.at[r, v], tx.at[r, v], fxs.at[0, 0], fxr.at[r, v], partner).wait_recv()
            total = total + tx[r, v].astype(F32)
        tflat[STEP * r : STEP * (r + 1), :] = total
    bcopies = []
    for s in range(8):
        zout[s] = tflat[MINI * s : MINI * (s + 1), :].astype(BF16)
        copy = send(
            zout.at[s], zback.at[zl], bs.at[s], br.at[zl], at(zl=4 * c + s // 2, c=s % 2)
        )
        bcopies.append(copy)

        @pl.when(jnp.logical_not(jnp.logical_and(mine, slot == s)))
        def _():
            copy.start()

    @pl.when(mine)
    def _():
        zback[zl] = zout[slot]

    for v in xnext:
        send(d_x.at[v], d_x.at[v], ds2.at[0], dr2.at[v], partner).wait_recv()
    total_d = d_x[0].astype(F32)
    for v in range(1, NX):
        total_d = total_d + d_x[v].astype(F32)
    d_z[zl] = total_d.astype(BF16)
    d3 = []
    for k in range(1, NZ):
        d3.append(
            send(d_z.at[zl], d_z.at[zl], ds3.at[k - 1], dr3.at[zl], at(zl=lax.rem(zl + k, NZ)))
        )
        d3[-1].start()

    for t in range(NZ):

        @pl.when(jnp.logical_not(jnp.logical_and(mine, zl == t)))
        def _():
            send(zback.at[t], zback.at[t], bs.at[0], br.at[t], partner).wait_recv()

    total = zback[0].astype(F32)
    for t in range(1, NZ):
        total = total + zback[t].astype(F32)
    tg[...] = total

    for k in range(1, NZ):
        v = lax.rem(zl + k, NZ)
        send(d_z.at[v], d_z.at[v], ds3.at[0], dr3.at[v], partner).wait_recv()
    total_d = d_z[0].astype(F32)
    for t in range(1, NZ):
        total_d = total_d + d_z[t].astype(F32)
    d_last[c] = total_d
    d4 = send(d_last.at[c], d_last.at[c], ds4, dr4.at[c], partner)
    d4.start()

    send(u_z.at[1 - zh], u_z.at[1 - zh], us2, ur2.at[1 - zh], partner).wait_recv()
    ug[...] = (u_z[0].astype(F32) + u_z[1].astype(F32)).reshape(2, RANK, WIDE)
    send(d_last.at[1 - c], d_last.at[1 - c], ds4, dr4.at[1 - c], partner).wait_recv()
    dg[...] = d_last[...]

    for t in range(NZ):

        @pl.when(jnp.logical_not(jnp.logical_and(mine, zl == t)))
        def _():
            zcopies[t].wait_send()

    for s in range(8):

        @pl.when(jnp.logical_not(jnp.logical_and(mine, slot == s)))
        def _():
            bcopies[s].wait_send()

    for target, copy in fxcopies:

        @pl.when(x != target)
        def _():
            copy.wait_send()

    for copy in (
        qcopies + xcopies + ccopies + [tcopy] + pcopies + scopies + gcopies + mcopies
        + fcopies + u1 + [d1] + d2 + [u2] + d3 + [d4]
    ):
        copy.wait_send()


def on_device(tokens, frozen_weight, adapter_down, adapter_up, magnitude, hidden_gradient):
    vmem = pl.BlockSpec(memory_space=pltpu.VMEM)
    dma = pltpu.SemaphoreType.DMA
    scratch = [
        pltpu.VMEM((8, MINI, WIDE), BF16),
        pltpu.VMEM((ROWS, WIDE), F32),
        pltpu.VMEM((8, ROWS, WIDE), BF16),
        pltpu.VMEM((8, 2, WIDE), F32),
        pltpu.VMEM((CHUNKS, 2 * RANK, BLOCK), BF16),
        pltpu.VMEM((2, 2 * RANK, WIDE), BF16),
        pltpu.VMEM((CHUNKS, NY, 2, STEP, WIDE), BF16),
        pltpu.VMEM((CHUNKS, 3, 2, STEP, WIDE), BF16),
        pltpu.VMEM((CHUNKS, 2, STEP, WIDE), BF16),
        pltpu.VMEM((CHUNKS, 2, STEP, WIDE), BF16),
        pltpu.VMEM((NH, ROWS, WIDE), BF16),
        pltpu.VMEM((CHUNKS, NY, 2, STEP, WIDE), BF16),
        pltpu.VMEM((2, WIDE), F32),
        pltpu.VMEM((NY, 2, WIDE), F32),
        pltpu.VMEM((2, RANK, WIDE), F32),
        pltpu.VMEM((2, RANK, WIDE), F32),
        pltpu.VMEM((2, RANK, WIDE), F32),
        pltpu.VMEM((CHUNKS, 2, 2, STEP, WIDE), BF16),
        pltpu.VMEM((CHUNKS, 2, STEP, WIDE), BF16),
        pltpu.VMEM((CHUNKS, 2, STEP, WIDE), BF16),
        pltpu.VMEM((PARTS, NX, STEP, WIDE), BF16),
        pltpu.VMEM((ROWS, WIDE), F32),
        pltpu.VMEM((8, MINI, WIDE), BF16),
        pltpu.VMEM((NZ, MINI, WIDE), BF16),
        pltpu.VMEM((RANK, WIDE), BF16),
        pltpu.VMEM((RANK, WIDE), BF16),
        pltpu.VMEM((NX, RANK, WIDE), BF16),
        pltpu.VMEM((NZ, RANK, WIDE), BF16),
        pltpu.VMEM((2, RANK, WIDE), F32),
        pltpu.VMEM((NY, 2 * RANK, WIDE), BF16),
        pltpu.VMEM((NH, 2 * RANK, WIDE), BF16),
        dma((NZ,)), dma((8,)),
        dma((3,)), dma((NX,)),
        dma((NX,)), dma((NX,)),
        dma((7,)), dma((8,)),
        dma, dma,
        dma((CHUNKS, 3)), dma((CHUNKS, 3)),
        dma((CHUNKS,)), dma((CHUNKS,)),
        dma((CHUNKS, 3)), dma((CHUNKS, NY)),
        dma((3,)), dma((NY,)),
        dma((CHUNKS, 2)), dma((CHUNKS, 2)),
        dma((CHUNKS, 2)), dma((PARTS, NX)),
        dma((8,)), dma((NZ,)),
        dma, dma,
        dma((3,)), dma((NX,)),
        dma((NZ - 1,)), dma((NZ,)),
        dma, dma((2,)),
        dma((3,)), dma((NY,)),
        dma, dma((NH,)),
    ]
    return pl.pallas_call(
        kernel,
        name="dora_step",
        out_shape=(
            jax.ShapeDtypeStruct((ROWS, WIDE), BF16),
            jax.ShapeDtypeStruct((MINI, WIDE), F32),
            jax.ShapeDtypeStruct((2, RANK, WIDE), F32),
            jax.ShapeDtypeStruct((2, RANK, WIDE), F32),
            jax.ShapeDtypeStruct((2, WIDE), F32),
        ),
        in_specs=[vmem] * 6,
        out_specs=(vmem,) * 5,
        scratch_shapes=scratch,
        compiler_params=pltpu.CompilerParams(
            collective_id=0, has_side_effects=True, vmem_limit_bytes=60 * 1024 * 1024
        ),
    )(tokens, frozen_weight, adapter_down, adapter_up, magnitude, hidden_gradient)


def solution(mesh):
    in_specs = (
        P("dp", "mp"),
        P(None, "mp", "dp"),
        P(None, None, "mp"),
        P(None, None, "dp"),
        P(None, "dp"),
        P("mp", "dp"),
    )
    out_specs = (
        P("mp", "dp"),
        P("dp", "mp"),
        P(None, None, "mp"),
        P(None, None, "dp"),
        P(None, "dp"),
    )
    return jax.shard_map(
        on_device, mesh=mesh, in_specs=in_specs, out_specs=out_specs, check_vma=False
    )
```

```python
import jax
import jax.numpy as jnp
from jax import lax
from jax.experimental import pallas as pl
from jax.experimental.pallas import tpu as pltpu
from jax.sharding import PartitionSpec as P

SCALE = 2.0
EPSILON = 1e-06
MESH = pl.DeviceIdType.MESH
F32 = jnp.float32
BF16 = jnp.bfloat16
NT = (((1,), (1,)), ((), ()))
TN = (((0,), (0,)), ((), ()))
NN = (((1,), (0,)), ((), ()))

NX, NY, NZ, NH, NC = 4, 4, 8, 2, 2
ROWS = 96
MINI = 12
WIDE = 576
RANK = 16
PIECES = ((0, 16), (16, 32), (48, 32), (80, 16))
LEAVES = ((0,), (1, 2, 3), (4, 5), (6, 7))
CHUNKS = len(PIECES) * NH
GROUPS = ((0, 16), (16, 80))
HALVES = ((0, 48), (48, 48))
ORDER = (
    "P0 P1 G P2 S0 P3 S1 P4 S2 P5 S3 H P6 S4 P7 S5 N C0 C1 S6 S7 B0 C2 B1 U0 C3 B2 U1 C4 B3 U2 V0 "
    "C5 B4 U3 C6 B5 U4 V1 C7 M B6 U5 W U6 B7 V2"
).split()


def dot(a, b, dims=NN):
    return lax.dot_general(a, b, dims, preferred_element_type=F32)


def wide_dot(a, b, dims=NN):
    total = None
    for _ in range(3):
        term = a.astype(BF16)
        a = a - term.astype(F32)
        value = dot(term, b, dims)
        total = value if total is None else total + value
    return total


def gelu_pair(source):
    square = source * source
    tangent = jnp.tanh(0.7978845608028654 * (source + 0.044715 * source * square))
    half = 0.5 * (1.0 + tangent)
    slope = half + 0.5 * source * (1.0 - tangent * tangent) * 0.7978845608028654 * (
        1.0 + 0.134145 * square
    )
    return source * half, slope


def kernel(
    tok_in, w_in, down_in, up_in, mag_in, cot_in,
    hid, tg, dg, ug, mg,
    tok, w, down, up, mag,
    zin, zflat, xb, sq, low_t, up_wide, part, ypart, zpart_out, zpart_in, cots, grad,
    mom, mom_all, acc_d, acc_u, cross, tb, tpair, tsum, tx, tflat, zout, zback,
    d_pair_out, d_pair_in, d_x_out, d_x, d_z, d_all, u_out, u_y, u_z, u_all,
    ls, zs, zr, xs, xr, cs, cr, qs, qr, ts, tr, answer, ps, pr, ss, sr, gs, gr, ms, mr,
    fs, fr, fxs, fxr, bs, br, ds1, dr1, ds2, dr2, ds3, dr3, ds4, dr4, us1, ur1, us2, ur2, us3, ur3,
):
    dp = lax.axis_index("dp")
    mp = lax.axis_index("mp")
    c = lax.rem(dp, NC)
    zl = lax.rem(dp // NC, NZ)
    x = dp // (NC * NZ)
    y = lax.rem(mp, NY)
    zh = mp // NY
    half = zl // 4
    slot = lax.rem(zl, 4) * 2 + c
    mine = half == c

    def at(x=x, zl=zl, c=c, zh=zh, y=y):
        return ((x * NZ + zl) * NC + c, zh * NY + y)

    def send(src, dst, s, r, device):
        return pltpu.make_async_remote_copy(
            src_ref=src, dst_ref=dst, send_sem=s, recv_sem=r,
            device_id=device, device_id_type=MESH,
        )

    partner = at(c=1 - c)
    across = at(zh=1 - zh)
    xnext = [lax.rem(x + d, NX) for d in range(1, NX)]
    ynext = [lax.rem(y + d, NY) for d in range(1, NY)]
    xdev = [at(x=v) for v in xnext]
    ydev = [at(y=v) for v in ynext]
    sent = []

    def go(src, dst, s, r, device):
        copy = send(src, dst, s, r, device)
        copy.start()
        sent.append(copy)

    def come(ref, s, r):
        send(ref, ref, s, r, partner).wait_recv()

    barrier = pltpu.get_barrier_semaphore()
    greeted = 0
    for k in range(1, NZ):
        for other in (c, 1 - c):
            pl.semaphore_signal(
                barrier, 1, device_id=at(zl=lax.rem(zl + k, NZ), c=other), device_id_type=MESH
            )
            greeted += 1
    far = [across] + [at(zh=1 - zh, y=v) for v in ynext]
    xpair = [at(x=v, c=1 - c) for v in xnext]
    for device in [partner] + xdev + ydev + xpair:
        pl.semaphore_signal(barrier, 1, device_id=device, device_id_type=MESH)
        greeted += 1

    @pl.when(zh == 0)
    def _():
        for device in far:
            pl.semaphore_signal(barrier, 1, device_id=device, device_id_type=MESH)

    local = [
        pltpu.make_async_copy(a, b, ls.at[i])
        for i, (a, b) in enumerate(
            ((down_in, down), (up_in, up), (w_in, w), (tok_in, tok), (mag_in, mag),
             (cot_in, cots.at[zh]))
        )
    ]
    for copy in local:
        copy.start()

    for copy in local:
        copy.wait()
    for k in range(2):
        merged = w[k].astype(F32) + SCALE * dot(down[k], up[k], TN)
        sq[mp, pl.ds(k, 1), :] = jnp.sum(merged * merged, axis=0, keepdims=True)

    @pl.when(zh == 0)
    def _():
        pl.semaphore_wait(barrier, greeted)

    @pl.when(zh == 1)
    def _():
        pl.semaphore_wait(barrier, greeted + len(far))
        for device in far:
            pl.semaphore_signal(answer, 1, device_id=device, device_id_type=MESH)

    zcopies = []
    for t in range(NZ):
        zcopies.append(send(tok, zin.at[slot], zs.at[t], zr.at[slot], at(zl=t, c=half)))

        @pl.when(jnp.logical_not(jnp.logical_and(mine, zl == t)))
        def _():
            zcopies[t].start()

    @pl.when(mine)
    def _():
        zin[slot] = tok[...]

    for i, device in enumerate(ydev):
        go(sq.at[mp], sq.at[mp], qs.at[i], qr.at[mp], device)

    for k in range(2):
        up_wide[k] = jnp.zeros((2 * RANK, WIDE), BF16)
        up_wide[k, RANK * k : RANK * (k + 1), :] = (SCALE * up[k].astype(F32)).astype(BF16)
        gram = dot(down[k], down[k], NT)
        cross[k] = dot(down[k], w[k]) + SCALE * wide_dot(gram, up[k])
    mom[...] = jnp.zeros_like(mom)
    acc_d[...] = jnp.zeros_like(acc_d)
    acc_u[...] = jnp.zeros_like(acc_u)
    down_both = down[...].reshape(2 * RANK, WIDE)

    for s in range(8):

        @pl.when(jnp.logical_not(jnp.logical_and(mine, slot == s)))
        def _():
            come(zin.at[s], zs.at[0], zr.at[s])

        zflat[MINI * s : MINI * (s + 1), :] = zin[s].astype(F32)
    own = x * 2 + c
    xb[own] = zflat[...].astype(BF16)

    def tokens_in(v, core, g):
        first, size = GROUPS[g]
        return xb.at[v * 2 + core, pl.ds(first, size)]

    for g in range(2):
        for d in range(3):
            go(tokens_in(x, c, g), tokens_in(x, c, g), xs.at[d, g], xr.at[x, g], xdev[d])
        go(tokens_in(x, c, g), tokens_in(x, c, g), cs.at[x, g], cr.at[x, g], partner)

    @pl.when(zh == 0)
    def _():
        pl.semaphore_wait(answer, len(far))

    for i, device in enumerate(far):
        go(sq.at[mp], sq.at[mp], qs.at[3 + i], qr.at[mp], device)

    def cotangent(g, which):
        first, size = HALVES[g]
        return cots.at[which, pl.ds(first, size)]

    go(cotangent(0, zh), cotangent(0, zh), ts.at[0], tr.at[0], across)

    def tokens_ready(g):
        for v in [lax.rem(x + 3, NX), xnext[0], xnext[1]]:
            come(tokens_in(v, c, g), xs.at[0, g], xr.at[v, g])
            go(tokens_in(v, c, g), tokens_in(v, c, g), cs.at[v, g], cr.at[v, g], partner)
        for v in range(NX):
            come(tokens_in(v, 1 - c, g), cs.at[0, g], cr.at[v, g])

    def place(q):
        first, size = PIECES[q // NH]
        return first, size, q % NH

    def rows_of(q):
        first, size, h = place(q)
        return xb[NY * h : NY * (h + 1), first : first + size, :].reshape(NY * size, WIDE)

    def products(q):
        first, size, h = place(q)
        rows = pl.ds(first, size)
        lhs = rows_of(q)
        low = dot(lhs, down_both, NT).astype(BF16)
        low_t[q, :, 0 : NY * size] = dot(down_both, lhs, NT).astype(BF16)
        for k in range(2):
            value = dot(lhs, w[k]) + dot(low, up_wide[k])
            part[h, :, k, rows] = value.astype(BF16).reshape(NY, size, WIDE)
        for d in range(3):
            go(
                part.at[h, ynext[d], :, rows], ypart.at[h, d, :, rows],
                ps.at[q, d], pr.at[q, d], ydev[d],
            )

    def over_y(q):
        first, size, h = place(q)
        rows = pl.ds(first, size)
        total = part[h, y, :, rows].astype(F32)
        for d in range(3):
            come(ypart.at[h, d, :, rows], ps.at[q, d], pr.at[q, d])
            total = total + ypart[h, d, :, rows].astype(F32)
        zpart_out[h, :, rows] = total.astype(BF16)
        go(zpart_out.at[h, :, rows], zpart_in.at[h, :, rows], ss.at[q], sr.at[q], across)

    def activate(q, norm, ratio):
        first, size, h = place(q)
        rows = pl.ds(first, size)
        come(zpart_in.at[h, :, rows], ss.at[q], sr.at[q])
        if q == 2 * NH:
            come(cotangent(1, 1 - zh), ts.at[1], tr.at[1])
        pre = [
            zpart_out[h, k, rows].astype(F32) + zpart_in[h, k, rows].astype(F32)
            for k in range(2)
        ]
        gate = pre[0] * ratio[0:1]
        lift = pre[1] * ratio[1:2]
        active, slope = gelu_pair(gate)

        @pl.when(zh == h)
        def _():
            hid[rows, :] = (active * lift).astype(BF16)

        g = cots[h, rows, :].astype(F32)
        outs = [g * lift * slope, g * active]
        for k in range(2):
            mom[k : k + 1, :] += jnp.sum(outs[k] * pre[k], axis=0, keepdims=True)
            grad[h, y, k, rows] = (outs[k] * ratio[k : k + 1]).astype(BF16)
        for d in range(3):
            go(
                grad.at[h, y, :, rows], grad.at[h, y, :, rows],
                gs.at[q, d], gr.at[q, y], ydev[d],
            )

    def backward(q):
        first, size, h = place(q)
        rows = pl.ds(first, size)
        for d in range(3):
            come(grad.at[h, ynext[d], :, rows], gs.at[q, d], gr.at[q, ynext[d]])
        lhs = rows_of(q)
        total = None
        for k in range(2):
            g = grad[h, :, k, rows].reshape(NY * size, WIDE)
            low = dot(g, up[k], NT).astype(BF16)
            low_rows = dot(up[k], g, NT).astype(BF16)
            value = dot(g, w[k], NT) + SCALE * dot(low, down[k])
            total = value if total is None else total + value
            acc_d[k] += dot(low_rows, lhs)
            acc_u[k] += dot(low_t[q, RANK * k : RANK * (k + 1), 0 : NY * size], g)
        tb[h, :, :, rows] = total.astype(BF16).reshape(2, 2, size, WIDE)
        go(tb.at[h, :, 1 - c, rows], tpair.at[h, :, rows], fs.at[q], fr.at[q], partner)

    along_x = []

    def over_cores(q):
        first, size, h = place(q)
        rows = pl.ds(first, size)
        come(tpair.at[h, :, rows], fs.at[q], fr.at[q])
        for j in range(2):
            tsum[h, j, rows] = (
                tb[h, j, c, rows].astype(F32) + tpair[h, j, rows].astype(F32)
            ).astype(BF16)
            target = NH * h + j
            copy = send(
                tsum.at[h, j, rows], tx.at[x, rows],
                fxs.at[q, j], fxr.at[q // NH, x], at(x=target),
            )
            along_x.append((target, copy))

            @pl.when(x != target)
            def _():
                copy.start()

    along_z = []

    def to_owner(p):
        first, size = PIECES[p]
        rows = pl.ds(first, size)
        total = tsum[x // 2, lax.rem(x, 2), rows].astype(F32)
        for v in xnext:
            come(tx.at[v, rows], fxs.at[0, 0], fxr.at[p, v])
            total = total + tx[v, rows].astype(F32)
        tflat[rows, :] = total
        for s in LEAVES[p]:
            zout[s] = tflat[MINI * s : MINI * (s + 1), :].astype(BF16)
            copy = send(
                zout.at[s], zback.at[zl], bs.at[s], br.at[zl], at(zl=4 * c + s // 2, c=s % 2)
            )
            along_z.append((s, copy))

            @pl.when(jnp.logical_not(jnp.logical_and(mine, slot == s)))
            def _():
                copy.start()

    tokens_ready(0)
    norm = ratio = None
    for item in ORDER:
        q = int(item[1:]) if len(item) > 1 else None
        if item == "G":
            tokens_ready(1)
        elif item == "N":
            for device in range(NH * NY):

                @pl.when(device != mp)
                def _():
                    come(sq.at[device], qs.at[0], qr.at[device])

            norm_square = sq[0]
            for device in range(1, NH * NY):
                norm_square = norm_square + sq[device]
            norm = jnp.sqrt(norm_square + EPSILON)
            ratio = mag[...] / norm
            come(cotangent(0, 1 - zh), ts.at[0], tr.at[0])
        elif item == "H":
            go(cotangent(1, zh), cotangent(1, zh), ts.at[1], tr.at[1], across)
        elif item == "M":
            mom_all[y] = mom[...]
            for d in range(3):
                go(mom_all.at[y], mom_all.at[y], ms.at[d], mr.at[y], ydev[d])
        elif item == "W":
            for v in ynext:
                come(mom_all.at[v], ms.at[0], mr.at[v])
            moment = mom_all[0]
            for v in range(1, NY):
                moment = moment + mom_all[v]
            mg[...] = moment / norm
            term = -mag[...] * moment / (norm * norm * norm)
            for k in range(2):
                acc_u[k] += cross[k] * term[k : k + 1]
                weighted = up[k].astype(F32) * term[k : k + 1]
                spread = wide_dot(weighted, w[k], NT)
                acc_d[k] += spread + SCALE * wide_dot(wide_dot(weighted, up[k], NT), down[k])
        elif item[0] == "P":
            products(q)
        elif item[0] == "S":
            over_y(q)
        elif item[0] == "C":
            activate(q, norm, ratio)
        elif item[0] == "B":
            backward(q)
        elif item[0] == "U":
            over_cores(q)
        else:
            to_owner(q)

    d_pair_out[...] = acc_d[1 - c].astype(BF16)
    go(d_pair_out, d_pair_in, ds1, dr1, partner)
    for k in range(2):
        u_out[2 * k : 2 * k + 2] = (SCALE * acc_u[k]).reshape(2, 8, WIDE)
    for d in range(3):
        go(u_out.at[ynext[d]], u_y.at[y], us1.at[d], ur1.at[y], ydev[d])
    u_y[y] = u_out[y]

    come(d_pair_in, ds1, dr1)
    total = SCALE * (acc_d[c] + d_pair_in[...].astype(F32))
    for i in range(NX):
        d_x_out[i] = total[4 * i : 4 * (i + 1)]
    for d in range(3):
        go(d_x_out.at[xnext[d]], d_x.at[x], ds2.at[d], dr2.at[x], xdev[d])
    d_x[x] = d_x_out[x]

    over_cores(CHUNKS - 1)

    for v in ynext:
        come(u_y.at[v], us1.at[0], ur1.at[v])
    total = u_y[0]
    for v in range(1, NY):
        total = total + u_y[v]
    u_z[zh] = total
    go(u_z.at[zh], u_z.at[zh], us2, ur2.at[zh], across)

    for v in xnext:
        come(d_x.at[v], ds2.at[0], dr2.at[v])
    total = d_x[0]
    for v in range(1, NX):
        total = total + d_x[v]
    d_z[zl] = total
    for k in range(1, NZ):
        go(d_z.at[zl], d_z.at[zl], ds3.at[k - 1], dr3.at[zl], at(zl=lax.rem(zl + k, NZ)))

    to_owner(len(PIECES) - 1)

    @pl.when(mine)
    def _():
        zback[zl] = zout[slot]

    for k in range(1, NZ):
        v = lax.rem(zl + k, NZ)
        come(d_z.at[v], ds3.at[0], dr3.at[v])
    total = d_z[0]
    for t in range(1, NZ):
        total = total + d_z[t]
    d_all[c, x] = total
    for i, device in enumerate([partner] + xdev + xpair):
        go(d_all.at[c, x], d_all.at[c, x], ds4.at[i], dr4.at[c, x], device)

    come(u_z.at[1 - zh], us2, ur2.at[1 - zh])
    u_all[y] = u_z[0] + u_z[1]
    for d in range(3):
        go(u_all.at[y], u_all.at[y], us3.at[d], ur3.at[y], ydev[d])

    for t in range(NZ):

        @pl.when(jnp.logical_not(jnp.logical_and(mine, zl == t)))
        def _():
            come(zback.at[t], bs.at[0], br.at[t])

    total = zback[0].astype(F32)
    for t in range(1, NZ):
        total = total + zback[t].astype(F32)
    tg[...] = total

    for v in ynext:
        come(u_all.at[v], us3.at[0], ur3.at[v])
    for k in range(2):
        ug[k] = u_all[2 * k : 2 * k + 2].reshape(RANK, WIDE)
    come(d_all.at[1 - c, x], ds4.at[0], dr4.at[1 - c, x])
    for v in xnext:
        for core in range(2):
            come(d_all.at[core, v], ds4.at[0], dr4.at[core, v])
    for k in range(2):
        for i in range(NX):
            dg[k, 4 * i : 4 * (i + 1), :] = d_all[k, i]

    for t in range(NZ):

        @pl.when(jnp.logical_not(jnp.logical_and(mine, zl == t)))
        def _():
            zcopies[t].wait_send()

    for s, copy in along_z:

        @pl.when(jnp.logical_not(jnp.logical_and(mine, slot == s)))
        def _():
            copy.wait_send()

    for target, copy in along_x:

        @pl.when(x != target)
        def _():
            copy.wait_send()

    for copy in sent:
        copy.wait_send()


def keep(*refs):
    for source, target in zip(refs[:5], refs[5:]):
        target[...] = source[...]


def on_device(tokens, frozen_weight, adapter_down, adapter_up, magnitude, hidden_gradient):
    vmem = pl.BlockSpec(memory_space=pltpu.VMEM)
    dma = pltpu.SemaphoreType.DMA
    scratch = [
        pltpu.VMEM((MINI, WIDE), BF16),
        pltpu.VMEM((2, WIDE, WIDE), BF16),
        pltpu.VMEM((2, RANK, WIDE), BF16),
        pltpu.VMEM((2, RANK, WIDE), BF16),
        pltpu.VMEM((2, WIDE), F32),
        pltpu.VMEM((8, MINI, WIDE), BF16),
        pltpu.VMEM((ROWS, WIDE), F32),
        pltpu.VMEM((8, ROWS, WIDE), BF16),
        pltpu.VMEM((8, 2, WIDE), F32),
        pltpu.VMEM((CHUNKS, 2 * RANK, 128), BF16),
        pltpu.VMEM((2, 2 * RANK, WIDE), BF16),
        pltpu.VMEM((NH, NY, 2, ROWS, WIDE), BF16),
        pltpu.VMEM((NH, 3, 2, ROWS, WIDE), BF16),
        pltpu.VMEM((NH, 2, ROWS, WIDE), BF16),
        pltpu.VMEM((NH, 2, ROWS, WIDE), BF16),
        pltpu.VMEM((NH, ROWS, WIDE), BF16),
        pltpu.VMEM((NH, NY, 2, ROWS, WIDE), BF16),
        pltpu.VMEM((2, WIDE), F32),
        pltpu.VMEM((NY, 2, WIDE), F32),
        pltpu.VMEM((2, RANK, WIDE), F32),
        pltpu.VMEM((2, RANK, WIDE), F32),
        pltpu.VMEM((2, RANK, WIDE), F32),
        pltpu.VMEM((NH, 2, 2, ROWS, WIDE), BF16),
        pltpu.VMEM((NH, 2, ROWS, WIDE), BF16),
        pltpu.VMEM((NH, 2, ROWS, WIDE), BF16),
        pltpu.VMEM((NX, ROWS, WIDE), BF16),
        pltpu.VMEM((ROWS, WIDE), F32),
        pltpu.VMEM((8, MINI, WIDE), BF16),
        pltpu.VMEM((NZ, MINI, WIDE), BF16),
        pltpu.VMEM((RANK, WIDE), BF16),
        pltpu.VMEM((RANK, WIDE), BF16),
        pltpu.VMEM((NX, 4, WIDE), F32),
        pltpu.VMEM((NX, 4, WIDE), F32),
        pltpu.VMEM((NZ, 4, WIDE), F32),
        pltpu.VMEM((2, NX, 4, WIDE), F32),
        pltpu.VMEM((NY, 8, WIDE), F32),
        pltpu.VMEM((NY, 8, WIDE), F32),
        pltpu.VMEM((NH, 8, WIDE), F32),
        pltpu.VMEM((NY, 8, WIDE), F32),
        dma((6,)),
        dma((NZ,)), dma((8,)),
        dma((3, 2)), dma((NX, 2)),
        dma((NX, 2)), dma((NX, 2)),
        dma((7,)), dma((8,)),
        dma((2,)), dma((2,)),
        pltpu.SemaphoreType.REGULAR,
        dma((CHUNKS, 3)), dma((CHUNKS, 3)),
        dma((CHUNKS,)), dma((CHUNKS,)),
        dma((CHUNKS, 3)), dma((CHUNKS, NY)),
        dma((3,)), dma((NY,)),
        dma((CHUNKS,)), dma((CHUNKS,)),
        dma((CHUNKS, 2)), dma((len(PIECES), NX)),
        dma((8,)), dma((NZ,)),
        dma, dma,
        dma((3,)), dma((NX,)),
        dma((NZ - 1,)), dma((NZ,)),
        dma((7,)), dma((2, NX)),
        dma((3,)), dma((NY,)),
        dma, dma((NH,)),
        dma((3,)), dma((NY,)),
    ]
    shapes = (
        jax.ShapeDtypeStruct((ROWS, WIDE), BF16),
        jax.ShapeDtypeStruct((MINI, WIDE), F32),
        jax.ShapeDtypeStruct((2, RANK, WIDE), F32),
        jax.ShapeDtypeStruct((2, RANK, WIDE), F32),
        jax.ShapeDtypeStruct((2, WIDE), F32),
    )
    results = pl.pallas_call(
        kernel,
        name="dora_step",
        out_shape=shapes,
        in_specs=[pl.BlockSpec(memory_space=pl.ANY)] * 6,
        out_specs=(vmem,) * 5,
        scratch_shapes=scratch,
        compiler_params=pltpu.CompilerParams(
            collective_id=0, has_side_effects=True, vmem_limit_bytes=60 * 1024 * 1024
        ),
    )(tokens, frozen_weight, adapter_down, adapter_up, magnitude, hidden_gradient)
    return pl.pallas_call(
        keep, name="keep", out_shape=shapes, in_specs=[vmem] * 5, out_specs=(vmem,) * 5
    )(*results)


def solution(mesh):
    in_specs = (
        P("dp", "mp"),
        P(None, "mp", "dp"),
        P(None, None, "mp"),
        P(None, None, "dp"),
        P(None, "dp"),
        P("mp", "dp"),
    )
    out_specs = (
        P("mp", "dp"),
        P("dp", "mp"),
        P(None, None, "mp"),
        P(None, None, "dp"),
        P(None, "dp"),
    )
    return jax.shard_map(
        on_device, mesh=mesh, in_specs=in_specs, out_specs=out_specs, check_vma=False
    )
```

```python
import jax
import jax.numpy as jnp
from jax import lax
from jax.experimental import pallas as pl
from jax.experimental.pallas import tpu as pltpu
from jax.sharding import PartitionSpec as P

SCALE = 2.0
EPSILON = 1e-06
MESH = pl.DeviceIdType.MESH
F32 = jnp.float32
BF16 = jnp.bfloat16
NT = (((1,), (1,)), ((), ()))
TN = (((0,), (0,)), ((), ()))
NN = (((1,), (0,)), ((), ()))

NX, NY, NZ, NH, NC = 4, 4, 8, 2, 2
ROWS = 96
MINI = 12
WIDE = 576
RANK = 16
PIECES = ((0, 16), (16, 16), (32, 16), (48, 16), (64, 16), (80, 16))
LEAVES = ((0,), (1,), (2, 3), (4,), (5,), (6, 7))
CHUNKS = len(PIECES) * NH
GROUPS = ((0, 16), (16, 80))
FAR_FIRST = (7, 0, 6, 1, 5, 2, 4, 3)
ORDER = (
    "P0 G P2 P4 S0 P6 S2 P8 P10 P1 S4 P3 S6 P5 S8 P7 S10 P9 P11 S1 N C0 S3 C1 S5 C2 S7 C3 S9 C4 "
    "S11 C5 B1 B3 U1 E0 B5 U3 E1 B7 U5 E2 B9 U7 B0 E3 B11 U9 B2 U11 U0 E4 B4 U2 W E5 B6 V0 U4 B8 V1 "
    "U6 B10"
).split()
LAG = 2


def dot(a, b, dims=NN):
    return lax.dot_general(a, b, dims, preferred_element_type=F32)


def wide_dot(a, b, dims=NN):
    total = None
    for _ in range(3):
        term = a.astype(BF16)
        a = a - term.astype(F32)
        value = dot(term, b, dims)
        total = value if total is None else total + value
    return total


def gelu_pair(source):
    square = source * source
    tangent = jnp.tanh(0.7978845608028654 * (source + 0.044715 * source * square))
    half = 0.5 * (1.0 + tangent)
    slope = half + 0.5 * source * (1.0 - tangent * tangent) * 0.7978845608028654 * (
        1.0 + 0.134145 * square
    )
    return source * half, slope


def kernel(
    tok_in, w_in, down_in, up_in, mag_in, cot_in,
    hid, tg, dg, ug, mg,
    tok, w, down, up, mag, cot,
    zin, zflat, xb, sq, low_t, up_wide, part, ypart, zpart_out, zpart_in, zown, grad,
    mom, mom_all, acc_d, acc_u, cross, tb, tpair, tsum, tx, tflat, zout, zback,
    d_x_out, d_x, d_z, d_all, u_out, u_y, u_z, u_all,
    ls, zs, zr, xs, xr, cs, cr, qs, qr, answer, ps, pr, ss, sr, gs, gr, gz, ms, mr,
    fs, fr, fxs, fxr, bs, br, ds2, dr2, ds3, dr3, ds4, dr4, us1, ur1, us2, ur2, us3, ur3,
):
    dp = lax.axis_index("dp")
    mp = lax.axis_index("mp")
    c = lax.rem(dp, NC)
    zl = lax.rem(dp // NC, NZ)
    x = dp // (NC * NZ)
    y = lax.rem(mp, NY)
    zh = mp // NY
    half = zl // 4
    slot = lax.rem(zl, 4) * 2 + c
    mine = half == c

    def at(x=x, zl=zl, c=c, zh=zh, y=y):
        return ((x * NZ + zl) * NC + c, zh * NY + y)

    def send(src, dst, s, r, device):
        return pltpu.make_async_remote_copy(
            src_ref=src, dst_ref=dst, send_sem=s, recv_sem=r,
            device_id=device, device_id_type=MESH,
        )

    partner = at(c=1 - c)
    across = at(zh=1 - zh)
    xnext = [lax.rem(x + d, NX) for d in range(1, NX)]
    ynext = [lax.rem(y + d, NY) for d in range(1, NY)]
    xdev = [at(x=v) for v in xnext]
    ydev = [at(y=v) for v in ynext]
    sent = []

    def go(src, dst, s, r, device):
        copy = send(src, dst, s, r, device)
        copy.start()
        sent.append(copy)

    def come(ref, s, r):
        send(ref, ref, s, r, partner).wait_recv()

    barrier = pltpu.get_barrier_semaphore()
    greeted = 0
    for k in range(1, NZ):
        for other in (c, 1 - c):
            pl.semaphore_signal(
                barrier, 1, device_id=at(zl=lax.rem(zl + k, NZ), c=other), device_id_type=MESH
            )
            greeted += 1
    far = [across] + [at(zh=1 - zh, y=v) for v in ynext]
    xpair = [at(x=v, c=1 - c) for v in xnext]
    for device in [partner] + xdev + ydev + xpair:
        pl.semaphore_signal(barrier, 1, device_id=device, device_id_type=MESH)
        greeted += 1

    @pl.when(zh == 0)
    def _():
        for device in far:
            pl.semaphore_signal(barrier, 1, device_id=device, device_id_type=MESH)

    local = [
        pltpu.make_async_copy(a, b, ls.at[i])
        for i, (a, b) in enumerate(
            ((down_in, down), (up_in, up), (w_in, w), (tok_in, tok), (mag_in, mag),
             (cot_in, cot))
        )
    ]
    for copy in local:
        copy.start()

    for copy in local:
        copy.wait()
    for k in range(2):
        merged = w[k].astype(F32) + SCALE * dot(down[k], up[k], TN)
        sq[mp, pl.ds(k, 1), :] = jnp.sum(merged * merged, axis=0, keepdims=True)

    @pl.when(zh == 0)
    def _():
        pl.semaphore_wait(barrier, greeted)

    @pl.when(zh == 1)
    def _():
        pl.semaphore_wait(barrier, greeted + len(far))
        for device in far:
            pl.semaphore_signal(answer, 1, device_id=device, device_id_type=MESH)

    zcopies = []
    for t in FAR_FIRST:
        copy = send(tok, zin.at[slot], zs.at[t], zr.at[slot], at(zl=t, c=half))
        zcopies.append((t, copy))

        @pl.when(jnp.logical_not(jnp.logical_and(mine, zl == t)))
        def _():
            copy.start()

    @pl.when(mine)
    def _():
        zin[slot] = tok[...]

    for i, device in enumerate(ydev):
        go(sq.at[mp], sq.at[mp], qs.at[i], qr.at[mp], device)

    for k in range(2):
        up_wide[k] = jnp.zeros((2 * RANK, WIDE), BF16)
        up_wide[k, RANK * k : RANK * (k + 1), :] = (SCALE * up[k].astype(F32)).astype(BF16)
        gram = dot(down[k], down[k], NT)
        cross[k] = dot(down[k], w[k]) + SCALE * wide_dot(gram, up[k])
    mom[...] = jnp.zeros_like(mom)
    acc_d[...] = jnp.zeros_like(acc_d)
    acc_u[...] = jnp.zeros_like(acc_u)
    down_both = down[...].reshape(2 * RANK, WIDE)

    for s in range(8):

        @pl.when(jnp.logical_not(jnp.logical_and(mine, slot == s)))
        def _():
            come(zin.at[s], zs.at[0], zr.at[s])

        zflat[MINI * s : MINI * (s + 1), :] = zin[s].astype(F32)
    own = x * 2 + c
    xb[own] = zflat[...].astype(BF16)

    def tokens_in(v, core, g):
        first, size = GROUPS[g]
        return xb.at[v * 2 + core, pl.ds(first, size)]

    for g in range(2):
        for d in range(3):
            go(tokens_in(x, c, g), tokens_in(x, c, g), xs.at[d, g], xr.at[x, g], xdev[d])
        go(tokens_in(x, c, g), tokens_in(x, c, g), cs.at[x, g], cr.at[x, g], partner)

    @pl.when(zh == 0)
    def _():
        pl.semaphore_wait(answer, len(far))

    for i, device in enumerate(far):
        go(sq.at[mp], sq.at[mp], qs.at[3 + i], qr.at[mp], device)

    def tokens_ready(g):
        for v in [lax.rem(x + 3, NX), xnext[0], xnext[1]]:
            come(tokens_in(v, c, g), xs.at[0, g], xr.at[v, g])
            go(tokens_in(v, c, g), tokens_in(v, c, g), cs.at[v, g], cr.at[v, g], partner)
        for v in range(NX):
            come(tokens_in(v, 1 - c, g), cs.at[0, g], cr.at[v, g])

    def place(q):
        return (q // 2, q % 2) + PIECES[q // 2]

    def rows_of(q):
        _, own_half, first, size = place(q)
        h = zh if own_half else 1 - zh
        return xb[pl.ds(NY * h, NY), first : first + size, :].reshape(NY * size, WIDE)

    def products(q):
        _, h, first, size = place(q)
        rows = pl.ds(first, size)
        lhs = rows_of(q)
        low = dot(lhs, down_both, NT).astype(BF16)
        low_t[q, :, 0 : NY * size] = dot(down_both, lhs, NT).astype(BF16)
        for k in range(2):
            value = dot(lhs, w[k]) + dot(low, up_wide[k])
            part[h, :, k, rows] = value.astype(BF16).reshape(NY, size, WIDE)
        for d in range(3):
            go(
                part.at[h, ynext[d], :, rows], ypart.at[h, d, :, rows],
                ps.at[q, d], pr.at[q, d], ydev[d],
            )

    def over_y(q):
        p, h, first, size = place(q)
        rows = pl.ds(first, size)
        total = part[h, y, :, rows].astype(F32)
        for d in range(3):
            come(ypart.at[h, d, :, rows], ps.at[q, d], pr.at[q, d])
            total = total + ypart[h, d, :, rows].astype(F32)
        if h:
            zown[:, rows] = total
        else:
            zpart_out[:, rows] = total.astype(BF16)
            go(zpart_out.at[:, rows], zpart_in.at[:, rows], ss.at[p], sr.at[p], across)

    def activate(p, norm, ratio):
        first, size = PIECES[p]
        rows = pl.ds(first, size)
        come(zpart_in.at[:, rows], ss.at[p], sr.at[p])
        pre = [zown[k, rows] + zpart_in[k, rows].astype(F32) for k in range(2)]
        gate = pre[0] * ratio[0:1]
        lift = pre[1] * ratio[1:2]
        active, slope = gelu_pair(gate)
        hid[rows, :] = (active * lift).astype(BF16)
        g = cot[rows, :].astype(F32)
        outs = [g * lift * slope, g * active]
        for k in range(2):
            mom[k : k + 1, :] += jnp.sum(outs[k] * pre[k], axis=0, keepdims=True)
            grad[1, y, k, rows] = (outs[k] * ratio[k : k + 1]).astype(BF16)
        block = grad.at[1, y, :, rows]
        for d in range(3):
            go(block, block, gs.at[2 * p + 1, d], gr.at[2 * p + 1, y], ydev[d])
        last = p == len(PIECES) - 1
        if last:
            mom_all[mp] = mom[...]
            for i, device in enumerate(far + ydev):
                go(mom_all.at[mp], mom_all.at[mp], ms.at[i], mr.at[mp], device)
        for v in range(max(p - LAG, 0) if last else p - LAG, p + 1 if last else p - LAG + 1):
            if v >= 0:
                back = pl.ds(*PIECES[v])
                go(
                    grad.at[1, y, :, back], grad.at[0, y, :, back],
                    gz.at[v], gr.at[2 * v, y], across,
                )

    def forward(p):
        block = grad.at[0, y, :, pl.ds(*PIECES[p])]
        come(block, gz.at[p], gr.at[2 * p, y])
        for d in range(3):
            go(block, block, gs.at[2 * p, d], gr.at[2 * p, y], ydev[d])

    def backward(q):
        _, h, first, size = place(q)
        rows = pl.ds(first, size)
        for d in range(3):
            come(grad.at[h, ynext[d], :, rows], gs.at[q, d], gr.at[q, ynext[d]])
        lhs = rows_of(q)
        total = None
        for k in range(2):
            g = grad[h, :, k, rows].reshape(NY * size, WIDE)
            low = dot(g, up[k], NT).astype(BF16)
            low_rows = dot(up[k], g, NT).astype(BF16)
            value = dot(g, w[k], NT) + SCALE * dot(low, down[k])
            total = value if total is None else total + value
            acc_d[k] += dot(low_rows, lhs)
            acc_u[k] += dot(low_t[q, RANK * k : RANK * (k + 1), 0 : NY * size], g)
        tb[h, :, :, rows] = total.astype(BF16).reshape(2, 2, size, WIDE)
        go(tb.at[h, :, 1 - c, rows], tpair.at[h, :, rows], fs.at[q], fr.at[q], partner)

    along_x = []

    def over_cores(q):
        p, h, first, size = place(q)
        rows = pl.ds(first, size)
        come(tpair.at[h, :, rows], fs.at[q], fr.at[q])
        for j in range(2):
            tsum[h, j, rows] = (
                tb[h, j, c, rows].astype(F32) + tpair[h, j, rows].astype(F32)
            ).astype(BF16)
            target = NH * (zh if h else 1 - zh) + j
            copy = send(
                tsum.at[h, j, rows], tx.at[x, rows],
                fxs.at[q, j], fxr.at[p, x], at(x=target),
            )
            along_x.append((target, copy))

            @pl.when(x != target)
            def _():
                copy.start()

    along_z = []

    def to_owner(p):
        first, size = PIECES[p]
        rows = pl.ds(first, size)
        total = tsum[1 - lax.rem(x // 2 + zh, 2), lax.rem(x, 2), rows].astype(F32)
        for v in xnext:
            come(tx.at[v, rows], fxs.at[0, 0], fxr.at[p, v])
            total = total + tx[v, rows].astype(F32)
        tflat[rows, :] = total
        for s in LEAVES[p]:
            zout[s] = tflat[MINI * s : MINI * (s + 1), :].astype(BF16)
            copy = send(
                zout.at[s], zback.at[zl], bs.at[s], br.at[zl], at(zl=4 * c + s // 2, c=s % 2)
            )
            along_z.append((s, copy))

            @pl.when(jnp.logical_not(jnp.logical_and(mine, slot == s)))
            def _():
                copy.start()

    tokens_ready(0)
    norm = ratio = None
    for item in ORDER:
        q = int(item[1:]) if len(item) > 1 else None
        if item == "G":
            tokens_ready(1)
        elif item == "N":
            for device in range(NH * NY):

                @pl.when(device != mp)
                def _():
                    come(sq.at[device], qs.at[0], qr.at[device])

            norm_square = sq[0]
            for device in range(1, NH * NY):
                norm_square = norm_square + sq[device]
            norm = jnp.sqrt(norm_square + EPSILON)
            ratio = mag[...] / norm
        elif item == "W":
            for device in range(NH * NY):

                @pl.when(device != mp)
                def _():
                    come(mom_all.at[device], ms.at[0], mr.at[device])

            moment = mom_all[0]
            for device in range(1, NH * NY):
                moment = moment + mom_all[device]
            mg[...] = moment / norm
            term = -mag[...] * moment / (norm * norm * norm)
            for k in range(2):
                acc_u[k] += cross[k] * term[k : k + 1]
                weighted = up[k].astype(F32) * term[k : k + 1]
                spread = wide_dot(weighted, w[k], NT)
                acc_d[k] += spread + SCALE * wide_dot(wide_dot(weighted, up[k], NT), down[k])
        elif item[0] == "P":
            products(q)
        elif item[0] == "S":
            over_y(q)
        elif item[0] == "C":
            activate(q, norm, ratio)
        elif item[0] == "E":
            forward(q)
        elif item[0] == "B":
            backward(q)
        elif item[0] == "U":
            over_cores(q)
        else:
            to_owner(q)

    for k in range(2):
        for i in range(NX):
            d_x_out[k, i] = SCALE * acc_d[k, 4 * i : 4 * (i + 1), :]
    d_x[c, x] = d_x_out[c, x]
    others = [(1 - c, x)] + [(c, v) for v in xnext] + [(1 - c, v) for v in xnext]
    for i, (core, v) in enumerate(others):
        go(d_x_out.at[core, v], d_x.at[c, x], ds2.at[i], dr2.at[c, x], at(x=v, c=core))
    for k in range(2):
        u_out[2 * k : 2 * k + 2] = (SCALE * acc_u[k]).reshape(2, 8, WIDE)
    for d in range(3):
        go(u_out.at[ynext[d]], u_y.at[y], us1.at[d], ur1.at[y], ydev[d])
    u_y[y] = u_out[y]

    for v in ynext:
        come(u_y.at[v], us1.at[0], ur1.at[v])
    total = u_y[0]
    for v in range(1, NY):
        total = total + u_y[v]
    u_z[zh] = total
    go(u_z.at[zh], u_z.at[zh], us2, ur2.at[zh], across)

    over_cores(CHUNKS - 4)
    over_cores(CHUNKS - 2)

    for core, v in others:
        come(d_x.at[core, v], ds2.at[0], dr2.at[core, v])
    total = d_x[0, 0]
    for i in range(1, NC * NX):
        total = total + d_x[i // NX, i % NX]
    d_z[zl] = total
    dcopies = []
    for t in FAR_FIRST:
        copy = send(d_z.at[zl], d_z.at[zl], ds3.at[t], dr3.at[zl], at(zl=t))
        dcopies.append((t, copy))

        @pl.when(zl != t)
        def _():
            copy.start()

    for p in range(2, len(PIECES) - 1):
        to_owner(p)
    to_owner(len(PIECES) - 1)

    @pl.when(mine)
    def _():
        zback[zl] = zout[slot]

    for k in range(1, NZ):
        v = lax.rem(zl + k, NZ)
        come(d_z.at[v], ds3.at[0], dr3.at[v])
    total = d_z[0]
    for t in range(1, NZ):
        total = total + d_z[t]
    d_all[c, x] = total
    for i, device in enumerate([partner] + xdev + xpair):
        go(d_all.at[c, x], d_all.at[c, x], ds4.at[i], dr4.at[c, x], device)

    come(u_z.at[1 - zh], us2, ur2.at[1 - zh])
    u_all[y] = u_z[0] + u_z[1]
    for d in range(3):
        go(u_all.at[y], u_all.at[y], us3.at[d], ur3.at[y], ydev[d])

    for t in range(NZ):

        @pl.when(jnp.logical_not(jnp.logical_and(mine, zl == t)))
        def _():
            come(zback.at[t], bs.at[0], br.at[t])

    total = zback[0].astype(F32)
    for t in range(1, NZ):
        total = total + zback[t].astype(F32)
    tg[...] = total

    for v in ynext:
        come(u_all.at[v], us3.at[0], ur3.at[v])
    for k in range(2):
        ug[k] = u_all[2 * k : 2 * k + 2].reshape(RANK, WIDE)
    come(d_all.at[1 - c, x], ds4.at[0], dr4.at[1 - c, x])
    for v in xnext:
        for core in range(2):
            come(d_all.at[core, v], ds4.at[0], dr4.at[core, v])
    for k in range(2):
        for i in range(NX):
            dg[k, 4 * i : 4 * (i + 1), :] = d_all[k, i]

    for t, copy in zcopies:

        @pl.when(jnp.logical_not(jnp.logical_and(mine, zl == t)))
        def _():
            copy.wait_send()

    for t, copy in dcopies:

        @pl.when(zl != t)
        def _():
            copy.wait_send()

    for s, copy in along_z:

        @pl.when(jnp.logical_not(jnp.logical_and(mine, slot == s)))
        def _():
            copy.wait_send()

    for target, copy in along_x:

        @pl.when(x != target)
        def _():
            copy.wait_send()

    for copy in sent:
        copy.wait_send()


def keep(*refs):
    for source, target in zip(refs[:5], refs[5:]):
        target[...] = source[...]


def on_device(tokens, frozen_weight, adapter_down, adapter_up, magnitude, hidden_gradient):
    vmem = pl.BlockSpec(memory_space=pltpu.VMEM)
    dma = pltpu.SemaphoreType.DMA
    scratch = [
        pltpu.VMEM((MINI, WIDE), BF16),
        pltpu.VMEM((2, WIDE, WIDE), BF16),
        pltpu.VMEM((2, RANK, WIDE), BF16),
        pltpu.VMEM((2, RANK, WIDE), BF16),
        pltpu.VMEM((2, WIDE), F32),
        pltpu.VMEM((ROWS, WIDE), BF16),
        pltpu.VMEM((8, MINI, WIDE), BF16),
        pltpu.VMEM((ROWS, WIDE), F32),
        pltpu.VMEM((8, ROWS, WIDE), BF16),
        pltpu.VMEM((8, 2, WIDE), F32),
        pltpu.VMEM((CHUNKS, 2 * RANK, 128), BF16),
        pltpu.VMEM((2, 2 * RANK, WIDE), BF16),
        pltpu.VMEM((NH, NY, 2, ROWS, WIDE), BF16),
        pltpu.VMEM((NH, 3, 2, ROWS, WIDE), BF16),
        pltpu.VMEM((2, ROWS, WIDE), BF16),
        pltpu.VMEM((2, ROWS, WIDE), BF16),
        pltpu.VMEM((2, ROWS, WIDE), F32),
        pltpu.VMEM((NH, NY, 2, ROWS, WIDE), BF16),
        pltpu.VMEM((2, WIDE), F32),
        pltpu.VMEM((8, 2, WIDE), F32),
        pltpu.VMEM((2, RANK, WIDE), F32),
        pltpu.VMEM((2, RANK, WIDE), F32),
        pltpu.VMEM((2, RANK, WIDE), F32),
        pltpu.VMEM((NH, 2, 2, ROWS, WIDE), BF16),
        pltpu.VMEM((NH, 2, ROWS, WIDE), BF16),
        pltpu.VMEM((NH, 2, ROWS, WIDE), BF16),
        pltpu.VMEM((NX, ROWS, WIDE), BF16),
        pltpu.VMEM((ROWS, WIDE), F32),
        pltpu.VMEM((8, MINI, WIDE), BF16),
        pltpu.VMEM((NZ, MINI, WIDE), BF16),
        pltpu.VMEM((2, NX, 4, WIDE), F32),
        pltpu.VMEM((2, NX, 4, WIDE), F32),
        pltpu.VMEM((NZ, 4, WIDE), F32),
        pltpu.VMEM((2, NX, 4, WIDE), F32),
        pltpu.VMEM((NY, 8, WIDE), F32),
        pltpu.VMEM((NY, 8, WIDE), F32),
        pltpu.VMEM((NH, 8, WIDE), F32),
        pltpu.VMEM((NY, 8, WIDE), F32),
        dma((6,)),
        dma((NZ,)), dma((8,)),
        dma((3, 2)), dma((NX, 2)),
        dma((NX, 2)), dma((NX, 2)),
        dma((7,)), dma((8,)),
        pltpu.SemaphoreType.REGULAR,
        dma((CHUNKS, 3)), dma((CHUNKS, 3)),
        dma((len(PIECES),)), dma((len(PIECES),)),
        dma((CHUNKS, 3)), dma((CHUNKS, NY)), dma((len(PIECES),)),
        dma((7,)), dma((8,)),
        dma((CHUNKS,)), dma((CHUNKS,)),
        dma((CHUNKS, 2)), dma((len(PIECES), NX)),
        dma((8,)), dma((NZ,)),
        dma((7,)), dma((2, NX)),
        dma((NZ,)), dma((NZ,)),
        dma((7,)), dma((2, NX)),
        dma((3,)), dma((NY,)),
        dma, dma((NH,)),
        dma((3,)), dma((NY,)),
    ]
    shapes = (
        jax.ShapeDtypeStruct((ROWS, WIDE), BF16),
        jax.ShapeDtypeStruct((MINI, WIDE), F32),
        jax.ShapeDtypeStruct((2, RANK, WIDE), F32),
        jax.ShapeDtypeStruct((2, RANK, WIDE), F32),
        jax.ShapeDtypeStruct((2, WIDE), F32),
    )
    results = pl.pallas_call(
        kernel,
        name="dora_step",
        out_shape=shapes,
        in_specs=[pl.BlockSpec(memory_space=pl.ANY)] * 6,
        out_specs=(vmem,) * 5,
        scratch_shapes=scratch,
        compiler_params=pltpu.CompilerParams(
            collective_id=0, has_side_effects=True, vmem_limit_bytes=60 * 1024 * 1024
        ),
    )(tokens, frozen_weight, adapter_down, adapter_up, magnitude, hidden_gradient)
    return pl.pallas_call(
        keep, name="keep", out_shape=shapes, in_specs=[vmem] * 5, out_specs=(vmem,) * 5
    )(*results)


def solution(mesh):
    in_specs = (
        P("dp", "mp"),
        P(None, "mp", "dp"),
        P(None, None, "mp"),
        P(None, None, "dp"),
        P(None, "dp"),
        P("mp", "dp"),
    )
    out_specs = (
        P("mp", "dp"),
        P("dp", "mp"),
        P(None, None, "mp"),
        P(None, None, "dp"),
        P(None, "dp"),
    )
    return jax.shard_map(
        on_device, mesh=mesh, in_specs=in_specs, out_specs=out_specs, check_vma=False
    )
```

```python
import jax
import jax.numpy as jnp
from jax import lax
from jax.experimental import pallas as pl
from jax.experimental.pallas import tpu as pltpu
from jax.sharding import PartitionSpec as P

SCALE = 2.0
EPSILON = 1e-06
MESH = pl.DeviceIdType.MESH
F32 = jnp.float32
BF16 = jnp.bfloat16
NT = (((1,), (1,)), ((), ()))
TN = (((0,), (0,)), ((), ()))
NN = (((1,), (0,)), ((), ()))

NX, NY, NZ, NH, NC = 4, 4, 8, 2, 2
ROWS = 96
MINI = 12
WIDE = 576
RANK = 16
PIECES = ((0, 16), (16, 16), (32, 16), (48, 16), (64, 16), (80, 16))
LEAVES = ((0,), (1,), (2, 3), (4,), (5,), (6, 7))
CHUNKS = len(PIECES) * NH
GROUPS = ((0, 16), (16, 80))
FAR_FIRST = (7, 0, 6, 1, 5, 2, 4, 3)
ORDER = (
    "P0 G P2 P4 S0 P6 S2 P8 P10 P1 S4 P3 S6 P5 S8 P7 S10 P9 P11 S1 N C0 S3 C1 S5 C2 S7 C3 S9 C4 "
    "S11 C5 B1 B3 U1 E0 B5 U3 E1 B7 U5 E2 B9 U7 B0 E3 B11 U9 B2 U11 U0 E4 B4 U2 W E5 B6 V0 U4 B8 V1 "
    "U6 B10"
).split()
CROSS = ((), (), (0,), (1, 2), (3, 4), (5,))


def dot(a, b, dims=NN):
    return lax.dot_general(a, b, dims, preferred_element_type=F32)


def wide_dot(a, b, dims=NN):
    total = None
    for _ in range(3):
        term = a.astype(BF16)
        a = a - term.astype(F32)
        value = dot(term, b, dims)
        total = value if total is None else total + value
    return total


def gelu_pair(source):
    square = source * source
    tangent = jnp.tanh(0.7978845608028654 * (source + 0.044715 * source * square))
    half = 0.5 * (1.0 + tangent)
    slope = half + 0.5 * source * (1.0 - tangent * tangent) * 0.7978845608028654 * (
        1.0 + 0.134145 * square
    )
    return source * half, slope


def kernel(
    tok_in, w_in, down_in, up_in, mag_in, cot_in,
    hid, tg, dg, ug, mg,
    tok, w, down, up, mag, cot,
    zin, zflat, xb, sq, low_t, up_wide, part, ypart, zpart_out, zpart_in, zown, grad,
    mom, mom_all, acc_d, acc_u, cross, tb, tpair, tsum, tx, tflat, zout, zback,
    d_x_out, d_x, d_z, d_all, u_out, u_y, u_z, u_all,
    ls, zs, zr, xs, xr, cs, cr, qs, qr, answer, ps, pr, ss, sr, gs, gr, gz, ms, mr,
    fs, fr, fxs, fxr, bs, br, ds2, dr2, ds3, dr3, ds4, dr4, us1, ur1, us2, ur2, us3, ur3,
):
    dp = lax.axis_index("dp")
    mp = lax.axis_index("mp")
    c = lax.rem(dp, NC)
    zl = lax.rem(dp // NC, NZ)
    x = dp // (NC * NZ)
    y = lax.rem(mp, NY)
    zh = mp // NY
    half = zl // 4
    slot = lax.rem(zl, 4) * 2 + c
    mine = half == c

    def at(x=x, zl=zl, c=c, zh=zh, y=y):
        return ((x * NZ + zl) * NC + c, zh * NY + y)

    def send(src, dst, s, r, device):
        return pltpu.make_async_remote_copy(
            src_ref=src, dst_ref=dst, send_sem=s, recv_sem=r,
            device_id=device, device_id_type=MESH,
        )

    partner = at(c=1 - c)
    across = at(zh=1 - zh)
    xnext = [lax.rem(x + d, NX) for d in range(1, NX)]
    ynext = [lax.rem(y + d, NY) for d in range(1, NY)]
    xdev = [at(x=v) for v in xnext]
    ydev = [at(y=v) for v in ynext]
    sent = []

    def go(src, dst, s, r, device):
        copy = send(src, dst, s, r, device)
        copy.start()
        sent.append(copy)

    def come(ref, s, r):
        send(ref, ref, s, r, partner).wait_recv()

    barrier = pltpu.get_barrier_semaphore()
    greeted = 0
    for k in range(1, NZ):
        for other in (c, 1 - c):
            pl.semaphore_signal(
                barrier, 1, device_id=at(zl=lax.rem(zl + k, NZ), c=other), device_id_type=MESH
            )
            greeted += 1
    far = [across] + [at(zh=1 - zh, y=v) for v in ynext]
    xpair = [at(x=v, c=1 - c) for v in xnext]
    for device in [partner] + xdev + ydev + xpair:
        pl.semaphore_signal(barrier, 1, device_id=device, device_id_type=MESH)
        greeted += 1

    @pl.when(zh == 0)
    def _():
        for device in far:
            pl.semaphore_signal(barrier, 1, device_id=device, device_id_type=MESH)

    local = [
        pltpu.make_async_copy(a, b, ls.at[i])
        for i, (a, b) in enumerate(
            ((tok_in, tok), (down_in, down), (up_in, up), (w_in, w), (mag_in, mag),
             (cot_in, cot))
        )
    ]
    for copy in local:
        copy.start()
    local[0].wait()

    @pl.when(zh == 0)
    def _():
        pl.semaphore_wait(barrier, greeted)

    @pl.when(zh == 1)
    def _():
        pl.semaphore_wait(barrier, greeted + len(far))
        for device in far:
            pl.semaphore_signal(answer, 1, device_id=device, device_id_type=MESH)

    zcopies = []
    for t in FAR_FIRST:
        copy = send(tok, zin.at[slot], zs.at[t], zr.at[slot], at(zl=t, c=half))
        zcopies.append((t, copy))

        @pl.when(jnp.logical_not(jnp.logical_and(mine, zl == t)))
        def _():
            copy.start()

    @pl.when(mine)
    def _():
        zin[slot] = tok[...]

    for copy in local[1:]:
        copy.wait()
    for k in range(2):
        merged = w[k].astype(F32) + SCALE * dot(down[k], up[k], TN)
        sq[mp, pl.ds(k, 1), :] = jnp.sum(merged * merged, axis=0, keepdims=True)

    for i, device in enumerate(ydev):
        go(sq.at[mp], sq.at[mp], qs.at[i], qr.at[mp], device)

    for k in range(2):
        up_wide[k] = jnp.zeros((2 * RANK, WIDE), BF16)
        up_wide[k, RANK * k : RANK * (k + 1), :] = (SCALE * up[k].astype(F32)).astype(BF16)
        gram = dot(down[k], down[k], NT)
        cross[k] = dot(down[k], w[k]) + SCALE * wide_dot(gram, up[k])
    mom[...] = jnp.zeros_like(mom)
    acc_d[...] = jnp.zeros_like(acc_d)
    acc_u[...] = jnp.zeros_like(acc_u)
    down_both = down[...].reshape(2 * RANK, WIDE)

    def tokens_in(v, core, g):
        first, size = GROUPS[g]
        return xb.at[v * 2 + core, pl.ds(first, size)]

    own = x * 2 + c
    for g in range(2):
        for s in range(2 * g, 2 + 6 * g):

            @pl.when(jnp.logical_not(jnp.logical_and(mine, slot == s)))
            def _():
                come(zin.at[s], zs.at[0], zr.at[s])

            zflat[MINI * s : MINI * (s + 1), :] = zin[s].astype(F32)
        first, size = GROUPS[g]
        rows = slice(first, first + size)
        xb[own, rows, :] = zflat[rows, :].astype(BF16)
        for d in range(3):
            go(tokens_in(x, c, g), tokens_in(x, c, g), xs.at[d, g], xr.at[x, g], xdev[d])
        go(tokens_in(x, c, g), tokens_in(x, c, g), cs.at[x, g], cr.at[x, g], partner)

    @pl.when(zh == 0)
    def _():
        pl.semaphore_wait(answer, len(far))

    for i, device in enumerate(far):
        go(sq.at[mp], sq.at[mp], qs.at[3 + i], qr.at[mp], device)

    def tokens_ready(g):
        for v in [lax.rem(x + 3, NX), xnext[0], xnext[1]]:
            come(tokens_in(v, c, g), xs.at[0, g], xr.at[v, g])
            go(tokens_in(v, c, g), tokens_in(v, c, g), cs.at[v, g], cr.at[v, g], partner)
        for v in range(NX):
            come(tokens_in(v, 1 - c, g), cs.at[0, g], cr.at[v, g])

    def place(q):
        return (q // 2, q % 2) + PIECES[q // 2]

    def rows_of(q):
        _, own_half, first, size = place(q)
        h = zh if own_half else 1 - zh
        return xb[pl.ds(NY * h, NY), first : first + size, :].reshape(NY * size, WIDE)

    def products(q):
        _, h, first, size = place(q)
        rows = pl.ds(first, size)
        lhs = rows_of(q)
        low = dot(lhs, down_both, NT).astype(BF16)
        low_t[q, :, 0 : NY * size] = dot(down_both, lhs, NT).astype(BF16)
        for k in range(2):
            value = dot(lhs, w[k]) + dot(low, up_wide[k])
            part[h, :, k, rows] = value.astype(BF16).reshape(NY, size, WIDE)
        for d in range(3):
            go(
                part.at[h, ynext[d], :, rows], ypart.at[h, d, :, rows],
                ps.at[q, d], pr.at[q, d], ydev[d],
            )

    def over_y(q):
        p, h, first, size = place(q)
        rows = pl.ds(first, size)
        total = part[h, y, :, rows].astype(F32)
        for d in range(3):
            come(ypart.at[h, d, :, rows], ps.at[q, d], pr.at[q, d])
            total = total + ypart[h, d, :, rows].astype(F32)
        if h:
            zown[:, rows] = total
        else:
            zpart_out[:, rows] = total.astype(BF16)
            go(zpart_out.at[:, rows], zpart_in.at[:, rows], ss.at[p], sr.at[p], across)

    def activate(p, norm, ratio):
        first, size = PIECES[p]
        rows = pl.ds(first, size)
        come(zpart_in.at[:, rows], ss.at[p], sr.at[p])
        pre = [zown[k, rows] + zpart_in[k, rows].astype(F32) for k in range(2)]
        gate = pre[0] * ratio[0:1]
        lift = pre[1] * ratio[1:2]
        active, slope = gelu_pair(gate)
        hid[rows, :] = (active * lift).astype(BF16)
        g = cot[rows, :].astype(F32)
        outs = [g * lift * slope, g * active]
        for k in range(2):
            mom[k : k + 1, :] += jnp.sum(outs[k] * pre[k], axis=0, keepdims=True)
            grad[1, y, k, rows] = (outs[k] * ratio[k : k + 1]).astype(BF16)
        block = grad.at[1, y, :, rows]
        for d in range(3):
            go(block, block, gs.at[2 * p + 1, d], gr.at[2 * p + 1, y], ydev[d])
        last = p == len(PIECES) - 1
        if last:
            mom_all[mp] = mom[...]
            for i, device in enumerate(far + ydev):
                go(mom_all.at[mp], mom_all.at[mp], ms.at[i], mr.at[mp], device)
        for v in CROSS[p]:
            back = pl.ds(*PIECES[v])
            go(
                grad.at[1, y, :, back], grad.at[0, y, :, back],
                gz.at[v], gr.at[2 * v, y], across,
            )

    def forward(p):
        block = grad.at[0, y, :, pl.ds(*PIECES[p])]
        come(block, gz.at[p], gr.at[2 * p, y])
        for d in range(3):
            go(block, block, gs.at[2 * p, d], gr.at[2 * p, y], ydev[d])

    def backward(q):
        _, h, first, size = place(q)
        rows = pl.ds(first, size)
        for d in range(3):
            come(grad.at[h, ynext[d], :, rows], gs.at[q, d], gr.at[q, ynext[d]])
        lhs = rows_of(q)
        total = None
        for k in range(2):
            g = grad[h, :, k, rows].reshape(NY * size, WIDE)
            low = dot(g, up[k], NT).astype(BF16)
            low_rows = dot(up[k], g, NT).astype(BF16)
            value = dot(g, w[k], NT) + SCALE * dot(low, down[k])
            total = value if total is None else total + value
            acc_d[k] += dot(low_rows, lhs)
            acc_u[k] += dot(low_t[q, RANK * k : RANK * (k + 1), 0 : NY * size], g)
        tb[h, :, :, rows] = total.astype(BF16).reshape(2, 2, size, WIDE)
        go(tb.at[h, :, 1 - c, rows], tpair.at[h, :, rows], fs.at[q], fr.at[q], partner)

    along_x = []

    def over_cores(q):
        p, h, first, size = place(q)
        rows = pl.ds(first, size)
        come(tpair.at[h, :, rows], fs.at[q], fr.at[q])
        for j in range(2):
            tsum[h, j, rows] = (
                tb[h, j, c, rows].astype(F32) + tpair[h, j, rows].astype(F32)
            ).astype(BF16)
            target = NH * (zh if h else 1 - zh) + j
            copy = send(
                tsum.at[h, j, rows], tx.at[x, rows],
                fxs.at[q, j], fxr.at[p, x], at(x=target),
            )
            along_x.append((target, copy))

            @pl.when(x != target)
            def _():
                copy.start()

    along_z = []

    def to_owner(p):
        first, size = PIECES[p]
        rows = pl.ds(first, size)
        total = tsum[1 - lax.rem(x // 2 + zh, 2), lax.rem(x, 2), rows].astype(F32)
        for v in xnext:
            come(tx.at[v, rows], fxs.at[0, 0], fxr.at[p, v])
            total = total + tx[v, rows].astype(F32)
        tflat[rows, :] = total
        for s in LEAVES[p]:
            zout[s] = tflat[MINI * s : MINI * (s + 1), :].astype(BF16)
            copy = send(
                zout.at[s], zback.at[zl], bs.at[s], br.at[zl], at(zl=4 * c + s // 2, c=s % 2)
            )
            along_z.append((s, copy))

            @pl.when(jnp.logical_not(jnp.logical_and(mine, slot == s)))
            def _():
                copy.start()

    tokens_ready(0)
    norm = ratio = None
    for item in ORDER:
        q = int(item[1:]) if len(item) > 1 else None
        if item == "G":
            tokens_ready(1)
        elif item == "N":
            for device in range(NH * NY):

                @pl.when(device != mp)
                def _():
                    come(sq.at[device], qs.at[0], qr.at[device])

            norm_square = sq[0]
            for device in range(1, NH * NY):
                norm_square = norm_square + sq[device]
            norm = jnp.sqrt(norm_square + EPSILON)
            ratio = mag[...] / norm
        elif item == "W":
            for device in range(NH * NY):

                @pl.when(device != mp)
                def _():
                    come(mom_all.at[device], ms.at[0], mr.at[device])

            moment = mom_all[0]
            for device in range(1, NH * NY):
                moment = moment + mom_all[device]
            mg[...] = moment / norm
            term = -mag[...] * moment / (norm * norm * norm)
            for k in range(2):
                acc_u[k] += cross[k] * term[k : k + 1]
                weighted = up[k].astype(F32) * term[k : k + 1]
                spread = wide_dot(weighted, w[k], NT)
                acc_d[k] += spread + SCALE * wide_dot(wide_dot(weighted, up[k], NT), down[k])
        elif item[0] == "P":
            products(q)
        elif item[0] == "S":
            over_y(q)
        elif item[0] == "C":
            activate(q, norm, ratio)
        elif item[0] == "E":
            forward(q)
        elif item[0] == "B":
            backward(q)
        elif item[0] == "U":
            over_cores(q)
        else:
            to_owner(q)

    for k in range(2):
        for i in range(NX):
            d_x_out[k, i] = SCALE * acc_d[k, 4 * i : 4 * (i + 1), :]
    d_x[c, x] = d_x_out[c, x]
    others = [(1 - c, x)] + [(c, v) for v in xnext] + [(1 - c, v) for v in xnext]
    for i, (core, v) in enumerate(others):
        go(d_x_out.at[core, v], d_x.at[c, x], ds2.at[i], dr2.at[c, x], at(x=v, c=core))
    for k in range(2):
        u_out[2 * k : 2 * k + 2] = (SCALE * acc_u[k]).reshape(2, 8, WIDE)
    for d in range(3):
        go(u_out.at[ynext[d]], u_y.at[y], us1.at[d], ur1.at[y], ydev[d])
    u_y[y] = u_out[y]

    for v in ynext:
        come(u_y.at[v], us1.at[0], ur1.at[v])
    total = u_y[0]
    for v in range(1, NY):
        total = total + u_y[v]
    u_z[zh] = total
    go(u_z.at[zh], u_z.at[zh], us2, ur2.at[zh], across)

    over_cores(CHUNKS - 4)
    over_cores(CHUNKS - 2)

    for core, v in others:
        come(d_x.at[core, v], ds2.at[0], dr2.at[core, v])
    total = d_x[0, 0]
    for i in range(1, NC * NX):
        total = total + d_x[i // NX, i % NX]
    d_z[zl] = total
    dcopies = []
    for t in FAR_FIRST:
        copy = send(d_z.at[zl], d_z.at[zl], ds3.at[t], dr3.at[zl], at(zl=t))
        dcopies.append((t, copy))

        @pl.when(zl != t)
        def _():
            copy.start()

    for p in range(2, len(PIECES) - 1):
        to_owner(p)
    to_owner(len(PIECES) - 1)

    @pl.when(mine)
    def _():
        zback[zl] = zout[slot]

    for k in range(1, NZ):
        v = lax.rem(zl + k, NZ)
        come(d_z.at[v], ds3.at[0], dr3.at[v])
    total = d_z[0]
    for t in range(1, NZ):
        total = total + d_z[t]
    d_all[c, x] = total
    for i, device in enumerate([partner] + xdev + xpair):
        go(d_all.at[c, x], d_all.at[c, x], ds4.at[i], dr4.at[c, x], device)

    come(u_z.at[1 - zh], us2, ur2.at[1 - zh])
    u_all[y] = u_z[0] + u_z[1]
    for d in range(3):
        go(u_all.at[y], u_all.at[y], us3.at[d], ur3.at[y], ydev[d])

    for t in range(NZ):

        @pl.when(jnp.logical_not(jnp.logical_and(mine, zl == t)))
        def _():
            come(zback.at[t], bs.at[0], br.at[t])

    total = zback[0].astype(F32)
    for t in range(1, NZ):
        total = total + zback[t].astype(F32)
    tg[...] = total

    for v in ynext:
        come(u_all.at[v], us3.at[0], ur3.at[v])
    for k in range(2):
        ug[k] = u_all[2 * k : 2 * k + 2].reshape(RANK, WIDE)
    come(d_all.at[1 - c, x], ds4.at[0], dr4.at[1 - c, x])
    for v in xnext:
        for core in range(2):
            come(d_all.at[core, v], ds4.at[0], dr4.at[core, v])
    for k in range(2):
        for i in range(NX):
            dg[k, 4 * i : 4 * (i + 1), :] = d_all[k, i]

    for t, copy in zcopies:

        @pl.when(jnp.logical_not(jnp.logical_and(mine, zl == t)))
        def _():
            copy.wait_send()

    for t, copy in dcopies:

        @pl.when(zl != t)
        def _():
            copy.wait_send()

    for s, copy in along_z:

        @pl.when(jnp.logical_not(jnp.logical_and(mine, slot == s)))
        def _():
            copy.wait_send()

    for target, copy in along_x:

        @pl.when(x != target)
        def _():
            copy.wait_send()

    for copy in sent:
        copy.wait_send()


def keep(*refs):
    for source, target in zip(refs[:5], refs[5:]):
        target[...] = source[...]


def on_device(tokens, frozen_weight, adapter_down, adapter_up, magnitude, hidden_gradient):
    vmem = pl.BlockSpec(memory_space=pltpu.VMEM)
    dma = pltpu.SemaphoreType.DMA
    scratch = [
        pltpu.VMEM((MINI, WIDE), BF16),
        pltpu.VMEM((2, WIDE, WIDE), BF16),
        pltpu.VMEM((2, RANK, WIDE), BF16),
        pltpu.VMEM((2, RANK, WIDE), BF16),
        pltpu.VMEM((2, WIDE), F32),
        pltpu.VMEM((ROWS, WIDE), BF16),
        pltpu.VMEM((8, MINI, WIDE), BF16),
        pltpu.VMEM((ROWS, WIDE), F32),
        pltpu.VMEM((8, ROWS, WIDE), BF16),
        pltpu.VMEM((8, 2, WIDE), F32),
        pltpu.VMEM((CHUNKS, 2 * RANK, 128), BF16),
        pltpu.VMEM((2, 2 * RANK, WIDE), BF16),
        pltpu.VMEM((NH, NY, 2, ROWS, WIDE), BF16),
        pltpu.VMEM((NH, 3, 2, ROWS, WIDE), BF16),
        pltpu.VMEM((2, ROWS, WIDE), BF16),
        pltpu.VMEM((2, ROWS, WIDE), BF16),
        pltpu.VMEM((2, ROWS, WIDE), F32),
        pltpu.VMEM((NH, NY, 2, ROWS, WIDE), BF16),
        pltpu.VMEM((2, WIDE), F32),
        pltpu.VMEM((8, 2, WIDE), F32),
        pltpu.VMEM((2, RANK, WIDE), F32),
        pltpu.VMEM((2, RANK, WIDE), F32),
        pltpu.VMEM((2, RANK, WIDE), F32),
        pltpu.VMEM((NH, 2, 2, ROWS, WIDE), BF16),
        pltpu.VMEM((NH, 2, ROWS, WIDE), BF16),
        pltpu.VMEM((NH, 2, ROWS, WIDE), BF16),
        pltpu.VMEM((NX, ROWS, WIDE), BF16),
        pltpu.VMEM((ROWS, WIDE), F32),
        pltpu.VMEM((8, MINI, WIDE), BF16),
        pltpu.VMEM((NZ, MINI, WIDE), BF16),
        pltpu.VMEM((2, NX, 4, WIDE), F32),
        pltpu.VMEM((2, NX, 4, WIDE), F32),
        pltpu.VMEM((NZ, 4, WIDE), F32),
        pltpu.VMEM((2, NX, 4, WIDE), F32),
        pltpu.VMEM((NY, 8, WIDE), F32),
        pltpu.VMEM((NY, 8, WIDE), F32),
        pltpu.VMEM((NH, 8, WIDE), F32),
        pltpu.VMEM((NY, 8, WIDE), F32),
        dma((6,)),
        dma((NZ,)), dma((8,)),
        dma((3, 2)), dma((NX, 2)),
        dma((NX, 2)), dma((NX, 2)),
        dma((7,)), dma((8,)),
        pltpu.SemaphoreType.REGULAR,
        dma((CHUNKS, 3)), dma((CHUNKS, 3)),
        dma((len(PIECES),)), dma((len(PIECES),)),
        dma((CHUNKS, 3)), dma((CHUNKS, NY)), dma((len(PIECES),)),
        dma((7,)), dma((8,)),
        dma((CHUNKS,)), dma((CHUNKS,)),
        dma((CHUNKS, 2)), dma((len(PIECES), NX)),
        dma((8,)), dma((NZ,)),
        dma((7,)), dma((2, NX)),
        dma((NZ,)), dma((NZ,)),
        dma((7,)), dma((2, NX)),
        dma((3,)), dma((NY,)),
        dma, dma((NH,)),
        dma((3,)), dma((NY,)),
    ]
    shapes = (
        jax.ShapeDtypeStruct((ROWS, WIDE), BF16),
        jax.ShapeDtypeStruct((MINI, WIDE), F32),
        jax.ShapeDtypeStruct((2, RANK, WIDE), F32),
        jax.ShapeDtypeStruct((2, RANK, WIDE), F32),
        jax.ShapeDtypeStruct((2, WIDE), F32),
    )
    results = pl.pallas_call(
        kernel,
        name="dora_step",
        out_shape=shapes,
        in_specs=[pl.BlockSpec(memory_space=pl.ANY)] * 6,
        out_specs=(vmem,) * 5,
        scratch_shapes=scratch,
        compiler_params=pltpu.CompilerParams(
            collective_id=0, has_side_effects=True, vmem_limit_bytes=60 * 1024 * 1024
        ),
    )(tokens, frozen_weight, adapter_down, adapter_up, magnitude, hidden_gradient)
    return pl.pallas_call(
        keep, name="keep", out_shape=shapes, in_specs=[vmem] * 5, out_specs=(vmem,) * 5
    )(*results)


def solution(mesh):
    in_specs = (
        P("dp", "mp"),
        P(None, "mp", "dp"),
        P(None, None, "mp"),
        P(None, None, "dp"),
        P(None, "dp"),
        P("mp", "dp"),
    )
    out_specs = (
        P("mp", "dp"),
        P("dp", "mp"),
        P(None, None, "mp"),
        P(None, None, "dp"),
        P(None, "dp"),
    )
    return jax.shard_map(
        on_device, mesh=mesh, in_specs=in_specs, out_specs=out_specs, check_vma=False
    )
```
